512 devices in a mesh: dp: 32 (over z, x), mp: 16 (over y, core).
Axes of the slice: x: 4, y: 8, z: 8, core: 2. Of those that a mesh axis runs over, the one named last changes fastest.
Arguments:
- hidden_acts: bfloat16 [32768, 8192], P('dp', 'mp'), may hold values from -12 to 12
- out_cotangent: bfloat16 [32768, 1024], P('dp'), may hold values from -0.003314563 to 0.003314563
- left_stats: float32 [128, 512, 512], P('dp', 'mp'), may hold values from -0.35355339 to 5.3535534
- right_stats: float32 [128, 512, 512], P('dp', 'mp'), may hold values from -0.35355339 to 5.3535534
- left_roots: bfloat16 [128, 512, 512], P('dp', 'mp'), may hold values from -0.088388348 to 1.0883883
- right_roots: bfloat16 [128, 512, 512], P('dp', 'mp'), may hold values from -0.088388348 to 1.0883883
- owner_map: int32 [32], replicated, may hold values from 0 to 31, as said below
- owner_counts: int32 [32], replicated, may hold values from 0 to 4, as said below
Outputs:
- update: bfloat16 [32, 512, 512], P('dp', 'mp')
- new_left: float32 [128, 512, 512], P('dp', 'mp')
- new_right: float32 [128, 512, 512], P('dp', 'mp')
The draws below stay inside these ranges and needn't reach their ends.
Inputs may be any that keep to these rules, and one draw needn't show every extreme that they name: owner_map[b] is the dp index that keeps block b's statistics; index d owns exactly owner_counts[d] blocks, at most 4, and some index owns exactly 4 in every draw. owner_counts[d] is the number of blocks b with owner_map[b] = d; the counts sum to 32.
All inputs are finite; a program needn't handle non-finite values.
Results may differ from the reference program's by a relative error of at most 0.018.
Values may be sent and summed in bfloat16 or wider, within the bound.
A program may use at most 64 MiB of HBM per device.

```python
import math
import jax
import jax.numpy as jnp
from jax import lax

BS = 512
NBC = 2
BPD = 1
TOK_DEV = 1024
CAP = 4
BLOCKS = 32
SLOTS = 128
NBR = 16
RB = 32
FW = 8192
DW = 1024
TOKENS = 32768
N_DP = 32
N_MP = 16


def column_scaled(key, rows, cols, factor):
    base_key, col_key = jax.random.split(key, 2)
    spread = jnp.exp(jax.random.uniform(col_key, (cols,), jnp.float32, math.log(0.3), math.log(3.0)))
    values = jnp.clip(jax.random.normal(base_key, (rows, cols), jnp.float32), -4.0, 4.0)
    return values * spread[None, :] * factor


def symmetric_slots(key, diagonal, spread):
    noise = jnp.clip(jax.random.normal(key, (SLOTS, BS, BS), jnp.float32), -4.0, 4.0)
    mixed = 0.5 * (noise + jnp.swapaxes(noise, 1, 2)) * (spread / math.sqrt(BS))
    return mixed + diagonal * jnp.eye(BS, dtype=jnp.float32)[None]


def owner_plan(key):
    base = jax.random.fold_in(key, 11)
    move_key, owner_key, block_key, flip_key = jax.random.split(base, 4)
    index_list = jnp.arange(N_DP, dtype=jnp.int32)
    counts = jnp.where(index_list == 0, 4 * BPD, jnp.where(index_list < 4, 0, BPD)).astype(jnp.int32)
    giver = (index_list >= 4) & ((index_list - 4) % 2 == 0) & (index_list + 1 < N_DP)
    moved = jnp.where(giver, jax.random.randint(move_key, (N_DP,), 0, BPD + 1, dtype=jnp.int32), 0).astype(jnp.int32)
    counts = counts - moved + jnp.roll(moved, 1)
    others = jnp.concatenate([jnp.arange(1, 5, dtype=jnp.int32), jnp.arange(6, N_DP, dtype=jnp.int32)])
    middle = (1 + jax.random.permutation(owner_key, N_DP - 2)).astype(jnp.int32)
    flip = jax.random.randint(flip_key, (), 0, 2, dtype=jnp.int32)
    first_end = (flip * (N_DP - 1)).astype(jnp.int32)
    second_end = ((1 - flip) * (N_DP - 1)).astype(jnp.int32)
    order = jnp.zeros((N_DP,), jnp.int32).at[others].set(middle).at[0].set(first_end).at[5].set(second_end)
    counts = jnp.zeros((N_DP,), jnp.int32).at[order].set(counts)
    ends = jnp.cumsum(counts).astype(jnp.int32)
    position = jnp.arange(BLOCKS, dtype=jnp.int32)
    sorted_owner = jnp.sum((ends[None, :] <= position[:, None]).astype(jnp.int32), axis=1)
    shuffle = jax.random.permutation(block_key, BLOCKS)
    assigned = sorted_owner[shuffle].astype(jnp.int32)
    first_owner = assigned[0]
    target = ((first_owner + 1) % N_DP).astype(jnp.int32)
    displaced = assigned[target]
    assigned = assigned.at[0].set(displaced).at[target].set(first_owner)
    return (assigned.astype(jnp.int32), counts.astype(jnp.int32))


def draw_hidden_acts(key, part):
    return column_scaled(jax.random.fold_in(key, 3), TOKENS, FW, 1.0).astype(jnp.bfloat16)


def draw_out_cotangent(key, part):
    return column_scaled(jax.random.fold_in(key, 5), TOKENS, DW, 0.05 / math.sqrt(TOKENS)).astype(jnp.bfloat16)


def draw_left_stats(key, part):
    return symmetric_slots(jax.random.fold_in(key, 7), 5.0, 2.0)


def draw_right_stats(key, part):
    return symmetric_slots(jax.random.fold_in(key, 13), 5.0, 2.0)


def draw_left_roots(key, part):
    return symmetric_slots(jax.random.fold_in(key, 17), 1.0, 0.5).astype(jnp.bfloat16)


def draw_right_roots(key, part):
    return symmetric_slots(jax.random.fold_in(key, 19), 1.0, 0.5).astype(jnp.bfloat16)


def draw_owner_map(key, part):
    return owner_plan(key)[0]


def draw_owner_counts(key, part):
    return owner_plan(key)[1]


def setup_inputs(seed: int = 0) -> dict:
    splits = jax.random.split(jax.random.key(seed), 9)
    hidden_acts = draw_hidden_acts(jax.random.fold_in(splits[8], 71), 0)
    out_cotangent = draw_out_cotangent(jax.random.fold_in(splits[8], 71), 0)
    left_stats = draw_left_stats(jax.random.fold_in(splits[8], 71), 0)
    right_stats = draw_right_stats(jax.random.fold_in(splits[8], 71), 0)
    left_roots = draw_left_roots(jax.random.fold_in(splits[8], 71), 0)
    right_roots = draw_right_roots(jax.random.fold_in(splits[8], 71), 0)
    owner_map = draw_owner_map(jax.random.fold_in(splits[8], 71), 0)
    owner_counts = draw_owner_counts(jax.random.fold_in(splits[8], 71), 0)
    return dict(hidden_acts=hidden_acts, out_cotangent=out_cotangent, left_stats=left_stats, right_stats=right_stats, left_roots=left_roots, right_roots=right_roots, owner_map=owner_map, owner_counts=owner_counts)


epsilon = 1e-06

def reference(hidden_acts, out_cotangent, left_stats, right_stats, left_roots, right_roots, owner_map, owner_counts):
    acts_split = hidden_acts.reshape(N_DP, TOK_DEV, FW)
    cotangents = out_cotangent.reshape(N_DP, TOK_DEV, DW)

    def accumulate(total_sum, act_pair):
        partial_value = lax.dot_general(act_pair[0], act_pair[1], (((0,), (0,)), ((), ())), preferred_element_type=jnp.float32)
        rounded = lax.optimization_barrier(partial_value.astype(jnp.bfloat16))
        return (total_sum + rounded.astype(jnp.float32), None)
    grad_sum, _ = lax.scan(accumulate, jnp.zeros((FW, DW), jnp.float32), (acts_split, cotangents))
    blocks = grad_sum.reshape(N_MP, NBR, RB, NBC, BS).transpose(1, 3, 0, 2, 4).reshape(BLOCKS, BS, BS)
    blocks = blocks.astype(jnp.bfloat16)
    block_ids = jnp.arange(BLOCKS, dtype=jnp.int32)
    same_owner = owner_map[:, None] == owner_map[None, :]
    owner_rank = lax.optimization_barrier(jnp.sum((same_owner & (block_ids[None, :] < block_ids[:, None])).astype(jnp.int32), axis=1)).astype(jnp.int32)
    is_live = (owner_rank < owner_counts[owner_map]) & (owner_rank < CAP)
    slot_of = jnp.where(is_live, owner_map * CAP + owner_rank, 0).astype(jnp.int32)

    def one_block(args):
        grad_block, where_slot, is_alive = args
        left_add = jnp.dot(grad_block, grad_block.T, preferred_element_type=jnp.float32)
        right_add = jnp.dot(grad_block.T, grad_block, preferred_element_type=jnp.float32)
        applied = jnp.dot(left_roots[where_slot], grad_block, preferred_element_type=jnp.float32).astype(jnp.bfloat16)
        conditioned = jnp.dot(applied, right_roots[where_slot], preferred_element_type=jnp.float32)
        widened = grad_block.astype(jnp.float32)
        scale_ratio = jnp.sqrt((jnp.mean(widened * widened) + epsilon) / (jnp.mean(conditioned * conditioned) + epsilon))
        keep_mask = is_alive.astype(jnp.float32)
        return (left_add * keep_mask, right_add * keep_mask, (conditioned * scale_ratio * keep_mask).astype(jnp.bfloat16))
    left_adds, right_adds, update = lax.map(one_block, (blocks, slot_of, is_live))
    slot_target = jnp.where(is_live, slot_of, SLOTS).astype(jnp.int32)
    new_left = left_stats.at[slot_target].add(left_adds, mode='drop')
    new_right = right_stats.at[slot_target].add(right_adds, mode='drop')
    return (update, new_left, new_right)
```

```python
import functools

import jax
import jax.numpy as jnp
from jax import lax
from jax.experimental import pallas as pl
from jax.experimental.pallas import tpu as pltpu
from jax.sharding import PartitionSpec as P

epsilon = 1e-06
COLS = 4
MESH = pl.DeviceIdType.MESH
f32, bf16 = jnp.float32, jnp.bfloat16


def kernel(
    sizes,
    tab,
    acts,
    cot,
    lstat,
    rstat,
    lroot,
    rroot,
    upd,
    new_left,
    new_right,
    a_v,
    at_v,
    c_v,
    ls_v,
    rs_v,
    lr_v,
    rr_v,
    part,
    q,
    rel,
    xa,
    fwd,
    xsum,
    zr,
    gful,
    rful,
    rxs,
    rx,
    rzs,
    rz,
    slab,
    cond_v,
    ssq_s,
    ssq,
    zb,
    fxs,
    fx,
    loc,
    s_rx,
    r_rx,
    s_rz,
    r_rz,
    s_x1,
    r_x1,
    s_x2,
    r_x2,
    s_z,
    r_z,
    s_y,
    r_y,
    s_c,
    r_c,
    s_q,
    r_q,
    s_f,
    r_f,
    s_fx,
    r_fx,
):
    nz, ny, mp, rows, width, cap = sizes
    dp = lax.axis_index("dp")
    m = lax.axis_index("mp")
    x, z = dp % COLS, dp // COLS
    c, y = m % 2, m // 2
    half = nz // 2

    def at_x(k):
        return {"dp": z * COLS + (x + k) % COLS}

    def at_z(k):
        return {"dp": ((z + k) % nz) * COLS + x}

    def at_y(k):
        return {"mp": ((y + k) % ny) * 2 + c}

    def at_m(k):
        return {"mp": (m + k) % mp}

    partner = {"mp": y * 2 + (1 - c)}

    def send(src, dst, ssem, rsem, where):
        return pltpu.make_async_remote_copy(
            src_ref=src,
            dst_ref=dst,
            send_sem=ssem,
            recv_sem=rsem,
            device_id=where,
            device_id_type=MESH,
        )

    def loop(lo, hi, body):
        def step(i, carry):
            body(i)
            return carry

        lax.fori_loop(lo, hi, step, 0)

    loads = [
        pltpu.make_async_copy(s, d, loc.at[i])
        for i, (s, d) in enumerate(
            [(lroot, lr_v), (rroot, rr_v), (acts, a_v), (cot, c_v), (lstat, ls_v), (rstat, rs_v)]
        )
    ]
    for copy in loads:
        copy.start()

    barrier = pltpu.get_barrier_semaphore()

    def hello(where):
        pl.semaphore_signal(barrier, inc=1, device_id=where, device_id_type=MESH)

    for k in range(1, COLS):
        hello(at_x(k))
    loop(1, nz, lambda k: hello(at_z(k)))
    loop(1, mp, lambda k: hello(at_m(k)))

    loads[0].wait()
    loads[1].wait()
    start_me = tab[1, dp]

    def slot_for(col):
        return (col + 4 * COLS * nz - start_me) % COLS

    for k in range(1, COLS):
        r = slot_for((x + k) % COLS)
        rxs[k - 1, 0] = lr_v[r]
        rxs[k - 1, 1] = rr_v[r]
    r = slot_for(x)
    rx[x, 0] = lr_v[r]
    rx[x, 1] = rr_v[r]
    pl.semaphore_wait(barrier, COLS - 1 + nz - 1 + mp - 1)
    root_x = [
        send(rxs.at[k - 1], rx.at[x], s_rx.at[k - 1], r_rx.at[k - 1], at_x(k)) for k in range(1, COLS)
    ]
    for copy in root_x:
        copy.start()

    loads[2].wait()
    tiles = a_v.shape[1] // 128

    def turn(i):
        at_v[pl.ds(i * 128, 128), :] = a_v[:, pl.ds(pl.multiple_of(i * 128, 128), 128)].T

    loop(0, tiles, turn)
    loads[3].wait()
    wide = 256
    per = width // wide

    def multiply(n):
        got = jnp.dot(
            at_v[...],
            c_v[:, pl.ds(pl.multiple_of(n * wide, wide), wide)],
            preferred_element_type=f32,
        )
        got = got.astype(bf16).reshape(part.shape[0], rows, wide)
        part[:, n // per, :, pl.ds(pl.multiple_of((n % per) * wide, wide), wide)] = got

    loop(0, c_v.shape[1] // wide, multiply)
    ncol = c_v.shape[1] // width

    def arrange(s):
        b = tab[2, s]
        q[s % COLS, s // COLS] = part[b // ncol, b % ncol]

    loop(0, COLS * nz, arrange)

    lo, hi = pl.ds(0, half), pl.ds(half, half)
    far, right, left = (x + 2) % COLS, (x + 1) % COLS, (x + 3) % COLS
    relay = [
        send(q.at[far, lo], rel.at[0], s_x1.at[0], r_x1.at[0], at_x(1)),
        send(q.at[far, hi], rel.at[1], s_x1.at[1], r_x1.at[1], at_x(3)),
    ]
    direct = [
        send(q.at[right, hi], xa.at[0], s_x1.at[2], r_x1.at[2], at_x(1)),
        send(q.at[left, lo], xa.at[1], s_x1.at[3], r_x1.at[3], at_x(3)),
    ]
    onward = [
        send(fwd.at[0], xa.at[2], s_x2.at[0], r_x2.at[0], at_x(1)),
        send(fwd.at[1], xa.at[3], s_x2.at[1], r_x2.at[1], at_x(3)),
    ]
    for copy in relay + direct:
        copy.start()

    for copy in root_x:
        copy.wait_recv()

    def root_row(k):
        row = (z + k) % nz
        xo = tab[3, row * COLS + x] % COLS
        rzs[row] = rx[xo]

    def root_send(k):
        return send(rzs.at[(z + k) % nz], rz.at[z], s_rz.at[k - 1], r_rz.at[k - 1], at_z(k))

    loop(0, nz, root_row)
    rz[z] = rzs[z]
    loop(1, nz, lambda k: root_send(k).start())

    for side, (toward, part_of) in enumerate([(right, lo), (left, hi)]):
        relay[side].wait_recv()
        fwd[side] = (q[toward, part_of].astype(f32) + rel[side].astype(f32)).astype(bf16)
        onward[side].start()
    for copy in direct + onward:
        copy.wait_recv()
    own = q[x].astype(f32)
    xsum[lo] = (own[:half] + xa[1].astype(f32) + xa[2].astype(f32)).astype(bf16)
    xsum[hi] = (own[half:] + xa[0].astype(f32) + xa[3].astype(f32)).astype(bf16)

    def z_send(k):
        return send(xsum.at[(z + k) % nz], zr.at[k - 1], s_z.at[k - 1], r_z.at[k - 1], at_z(k))

    loop(1, nz, lambda k: z_send(k).start())

    loop(1, nz, lambda k: root_send(k).wait_recv())
    source = tab[3, dp] // COLS
    rful[m] = rz[source, 1]

    def gather(full, which):
        def out(k):
            return send(full.at[m], full.at[m], s_y.at[which, k], r_y.at[which, k], at_y(k))

        def across(k):
            at = ((y + ny - k) % ny) * 2 + c
            return send(full.at[at], full.at[at], s_c.at[which, k], r_c.at[which, k], partner)

        return out, across

    r_out, r_across = gather(rful, 0)
    g_out, g_across = gather(gful, 1)
    loop(1, ny, lambda k: r_out(k).start())
    r_across(0).start()

    loop(1, nz, lambda k: z_send(k).wait_recv())
    total = xsum[z].astype(f32)
    for k in range(nz - 1):
        total = total + zr[k].astype(f32)
    gful[m] = total.astype(bf16)
    loop(1, ny, lambda k: g_out(k).start())
    g_across(0).start()

    def pass_on(out, across):
        def step(k):
            out(k).wait_recv()
            across(k).start()

        return step

    loop(1, ny, pass_on(r_out, r_across))
    loop(1, ny, pass_on(g_out, g_across))
    loop(0, ny, lambda k: r_across(k).wait_recv())
    loop(0, ny, lambda k: g_across(k).wait_recv())

    order = mp * rows
    g = gful[...].reshape(order, width)
    mine = gful[m]
    zb[0, z] = lax.dot_general(
        mine, g, (((1,), (1,)), ((), ())), preferred_element_type=f32
    ).astype(bf16)

    def ring(ch, h, way):
        if way == 0:
            at = (z + nz - (h - 1)) % nz
            return send(zb.at[ch, at], zb.at[ch, at], s_f.at[ch, way, h], r_f.at[ch, way, h], at_z(1))
        at = (z + (h - 1)) % nz
        return send(
            zb.at[ch, at], zb.at[ch, at], s_f.at[ch, way, h], r_f.at[ch, way, h], at_z(nz - 1)
        )

    hops = (nz // 2, nz - 1 - nz // 2)

    def ring_start(ch, h):
        for way in range(2):
            if h <= hops[way]:
                ring(ch, h, way).start()

    def ring_recv(ch, h):
        for way in range(2):
            if h <= hops[way]:
                ring(ch, h, way).wait_recv()

    ring_start(0, 1)
    piece = pl.multiple_of((m * rows // 128) * 128, 128)
    columns = gful[:, :, pl.ds(piece, 128)].reshape(order, 128)
    slab[...] = lax.dot_general(columns, g, (((0,), (0,)), ((), ())), preferred_element_type=f32)
    zb[1, z] = slab[pl.ds((m * rows) % 128, rows), :].astype(bf16)
    ring_start(1, 1)
    applied = jnp.dot(rz[source, 0], g, preferred_element_type=f32).astype(bf16)
    cond = jnp.dot(applied, rful[...].reshape(order, width), preferred_element_type=f32)
    cond_v[...] = cond
    partial_sum = jnp.broadcast_to(jnp.sum(cond * cond, keepdims=True), ssq_s.shape)
    ssq_s[...] = partial_sum
    ssq[m] = partial_sum

    def square_send(k):
        return send(ssq_s, ssq.at[m], s_q.at[k - 1], r_q.at[k - 1], at_m(k))

    loop(1, mp, lambda k: square_send(k).start())
    wide_g = g.astype(f32)
    grad_square = jnp.sum(wide_g * wide_g, keepdims=True)
    loop(1, mp, lambda k: square_send(k).wait_recv())
    cond_square = jnp.sum(ssq[...], axis=0)[0:1, 0:1]
    entries = float(order * width)
    ratio = jnp.sqrt((grad_square / entries + epsilon) / (cond_square / entries + epsilon))
    zb[2, z] = (cond_v[...] * ratio).astype(bf16)
    ring_start(2, 1)
    for h in range(1, hops[0] + 1):
        for ch in range(3):
            ring_recv(ch, h)
            if h < hops[0]:
                ring_start(ch, h + 1)

    def pick(col, place):
        o = z * COLS + col
        begin = tab[1, o]
        k = (begin + (x + 4 * COLS * nz - begin) % COLS) // COLS
        k = jnp.minimum(k, nz - 1)
        place[0] = zb[0, k]
        place[1] = zb[1, k]
        place[2] = zb[2, tab[0, o] // COLS]

    fin = []
    for k in range(1, COLS):
        pick((x + k) % COLS, fxs.at[k - 1])
        copy = send(fxs.at[k - 1], fx.at[x], s_fx.at[k - 1], r_fx.at[k - 1], at_x(k))
        copy.start()
        fin.append(copy)
    pick(x, fx.at[x])
    for copy in fin:
        copy.wait_recv()
    loads[4].wait()
    loads[5].wait()
    limit = tab[4, dp]
    for r in range(cap):
        col = (start_me + r) % COLS
        live = limit > r
        new_left[r] = ls_v[r] + jnp.where(live, fx[col, 0].astype(f32), 0.0)
        new_right[r] = rs_v[r] + jnp.where(live, fx[col, 1].astype(f32), 0.0)
    home = fx[tab[0, dp] % COLS, 2].astype(f32)
    upd[0] = jnp.where(tab[5, dp] > 0, home, 0.0).astype(bf16)

    for copy in root_x + relay + direct + onward + fin:
        copy.wait_send()
    loop(1, nz, lambda k: root_send(k).wait_send())
    loop(1, nz, lambda k: z_send(k).wait_send())
    loop(1, ny, lambda k: r_out(k).wait_send())
    loop(1, ny, lambda k: g_out(k).wait_send())
    loop(0, ny, lambda k: r_across(k).wait_send())
    loop(0, ny, lambda k: g_across(k).wait_send())
    loop(1, mp, lambda k: square_send(k).wait_send())
    for ch in range(3):
        for way in range(2):
            for h in range(1, hops[way] + 1):
                ring(ch, h, way).wait_send()


def tables(owner_map, owner_counts, capacity):
    blocks = owner_map.shape[0]
    ids = jnp.arange(blocks, dtype=jnp.int32)
    earlier = ids[None, :] < ids[:, None]
    same = owner_map[None, :] == owner_map[:, None]
    rank = jnp.sum((same & earlier).astype(jnp.int32), axis=1)
    before = jnp.sum((owner_map[None, :] < owner_map[:, None]).astype(jnp.int32), axis=1)
    place = before + rank
    begin = jnp.sum((owner_map[None, :] < ids[:, None]).astype(jnp.int32), axis=1)
    owned = jnp.sum((owner_map[None, :] == ids[:, None]).astype(jnp.int32), axis=1)
    limit = jnp.minimum(jnp.minimum(owned, owner_counts), capacity)
    held = jnp.sum(jnp.where(owner_map[:, None] == ids[None, :], owner_counts[None, :], 0), axis=1)
    live = ((rank < held) & (rank < capacity)).astype(jnp.int32)
    at = place[None, :] == ids[:, None]
    block_at = jnp.sum(jnp.where(at, ids[None, :], 0), axis=1)
    owner_at = jnp.sum(jnp.where(at, owner_map[None, :], 0), axis=1)
    return jnp.stack([place, begin, block_at, owner_at, limit, live])


def shards(acts, cot, lstat, rstat, lroot, rroot, owner_map, owner_counts):
    cap, rows, width = lstat.shape
    tok, own = acts.shape
    dw = cot.shape[1]
    devices, mp = lax.axis_size("dp"), lax.axis_size("mp")
    nz, ny = devices // COLS, mp // 2
    tab = tables(owner_map, owner_counts, cap)
    sizes = (nz, ny, mp, rows, width, cap)
    V, D = pltpu.VMEM, pltpu.SemaphoreType.DMA
    half = nz // 2

    def pieces(*lead):
        return V((*lead, rows, width), bf16)

    scratch = [
        V((tok, own), bf16),
        V((own, tok), bf16),
        V((tok, dw), bf16),
        V(lstat.shape, f32),
        V(rstat.shape, f32),
        V(lroot.shape, bf16),
        V(rroot.shape, bf16),
        pieces(own // rows, dw // width),
        pieces(COLS, nz),
        pieces(2, half),
        pieces(4, half),
        pieces(2, half),
        pieces(nz),
        pieces(nz - 1),
        pieces(mp),
        pieces(mp),
        pieces(COLS - 1, 2),
        pieces(COLS, 2),
        pieces(nz, 2),
        pieces(nz, 2),
        V((128, width), f32),
        V((rows, width), f32),
        V((8, 128), f32),
        V((mp, 8, 128), f32),
        pieces(3, nz),
        pieces(COLS - 1, 3),
        pieces(COLS, 3),
        D((6,)),
    ]
    for shape in [
        (COLS - 1,),
        (nz - 1,),
        (4,),
        (2,),
        (nz - 1,),
        (2, ny),
        (2, ny),
        (mp - 1,),
        (3, 2, nz),
        (COLS - 1,),
    ]:
        scratch += [D(shape), D(shape)]
    anywhere = pl.BlockSpec(memory_space=pl.ANY)
    vmem = pl.BlockSpec(memory_space=pltpu.VMEM)
    return pl.pallas_call(
        functools.partial(kernel, sizes),
        out_shape=(
            jax.ShapeDtypeStruct((1, rows, width), bf16),
            jax.ShapeDtypeStruct(lstat.shape, f32),
            jax.ShapeDtypeStruct(rstat.shape, f32),
        ),
        in_specs=[pl.BlockSpec(memory_space=pltpu.SMEM)] + [anywhere] * 6,
        out_specs=(vmem,) * 3,
        scratch_shapes=scratch,
        compiler_params=pltpu.CompilerParams(
            collective_id=0, has_side_effects=True, vmem_limit_bytes=40 << 20
        ),
        name="shampoo",
    )(tab, acts, cot, lstat, rstat, lroot, rroot)


def solution(mesh):
    in_specs = (
        P("dp", "mp"),
        P("dp", None),
        P("dp", "mp", None),
        P("dp", "mp", None),
        P("dp", "mp", None),
        P("dp", "mp", None),
        P(),
        P(),
    )
    out_specs = (P("dp", "mp", None), P("dp", "mp", None), P("dp", "mp", None))
    return jax.shard_map(shards, mesh=mesh, in_specs=in_specs, out_specs=out_specs, check_vma=False)
```

```python
import functools

import jax
import jax.numpy as jnp
from jax import lax
from jax.experimental import pallas as pl
from jax.experimental.pallas import tpu as pltpu
from jax.sharding import PartitionSpec as P

epsilon = 1e-06
COLS = 4
MESH = pl.DeviceIdType.MESH
PLANS = {
    1: (),
    2: ((0, 0, 1, False),),
    4: ((0, 0, 1, True), (0, 0, 2, False)),
    8: ((0, 0, 1, True), (0, 0, 2, True), (1, 2, 1, True), (1, 2, 2, False)),
}
f32, bf16 = jnp.float32, jnp.bfloat16


def kernel(
    sizes,
    omap,
    counts,
    acts,
    cot,
    lstat,
    rstat,
    lroot,
    rroot,
    upd,
    new_left,
    new_right,
    tab_v,
    tab,
    a_v,
    at_v,
    c_v,
    ls_v,
    rs_v,
    lr_v,
    rr_v,
    part,
    q,
    rel,
    xa,
    fwd,
    xsum,
    zr,
    gful,
    rful,
    rxs,
    rx_l,
    rx_r,
    rzs,
    rz_l,
    rz_r,
    zrel,
    zfwd,
    slab,
    cond_v,
    ssq_s,
    ssq,
    zb_l,
    zb_r,
    zb_u,
    fxs,
    fxs_u,
    fx,
    fx_u,
    loc,
    s_rx,
    r_rx,
    s_rz,
    r_rz,
    s_x,
    r_x,
    s_z,
    r_z,
    s_y,
    r_y,
    s_c,
    r_c,
    s_q,
    r_q,
    s_f,
    r_f,
    s_fx,
    r_fx,
):
    nz, ny, mp, rows, width, cap = sizes
    dp = lax.axis_index("dp")
    m = lax.axis_index("mp")
    x, z = dp % COLS, dp // COLS
    c, y = m % 2, m // 2
    half = nz // 2
    rx, rz, zb = (rx_l, rx_r), (rz_l, rz_r), (zb_l, zb_r, zb_u)
    part_rows = [pl.ds(h * (rows // 2), rows // 2) for h in range(2)]

    def at_x(k):
        return {"dp": z * COLS + (x + k) % COLS}

    def at_z(k):
        return {"dp": ((z + k) % nz) * COLS + x}

    def at_y(k):
        return {"mp": ((y + k) % ny) * 2 + c}

    def at_m(k):
        return {"mp": (m + k) % mp}

    partner = {"mp": y * 2 + (1 - c)}

    def send(src, dst, ssem, rsem, where):
        return pltpu.make_async_remote_copy(
            src_ref=src,
            dst_ref=dst,
            send_sem=ssem,
            recv_sem=rsem,
            device_id=where,
            device_id_type=MESH,
        )

    def loop(lo, hi, body):
        def step(i, carry):
            body(i)
            return carry

        lax.fori_loop(lo, hi, step, 0)

    def spread(pos, n, where, ref, ssem, rsem):
        plan = PLANS[n]

        def copy(i, way):
            _, behind, hop, whole = plan[i]
            origin = (pos + n - behind) % n if way == 0 else (pos + behind) % n
            r = ref(origin, None if whole else way)
            return send(
                r, r, ssem.at[way, i], rsem.at[way, i], where(hop if way == 0 else n - hop)
            )

        def start(stage):
            for i, item in enumerate(plan):
                if item[0] == stage:
                    for way in range(2):
                        copy(i, way).start()

        def forward():
            if len(plan) > 2:
                for way in range(2):
                    copy(1, way).wait_recv()
                start(1)

        def finish(arrived=None):
            for i, item in enumerate(plan):
                for way in range(2):
                    if not (len(plan) > 2 and i == 1):
                        copy(i, way).wait_recv()
                if arrived is not None:
                    far = item[1] + item[2]
                    arrived(far)
                    if item[3]:
                        arrived(n - far)

        def drain():
            for i in range(len(plan)):
                for way in range(2):
                    copy(i, way).wait_send()

        return start, forward, finish, drain

    barrier = pltpu.get_barrier_semaphore()

    def hello(where):
        pl.semaphore_signal(barrier, inc=1, device_id=where, device_id_type=MESH)

    loads = [
        pltpu.make_async_copy(s, d, loc.at[i])
        for i, (s, d) in enumerate(
            [(lroot, lr_v), (rroot, rr_v), (acts, a_v), (cot, c_v), (lstat, ls_v), (rstat, rs_v)]
        )
    ]
    for i in (2, 3, 1, 0):
        loads[i].start()
    for k in range(1, COLS):
        hello(at_x(k))
    loop(1, nz, lambda k: hello(at_z(k)))
    loop(1, mp, lambda k: hello(at_m(k)))

    tables(omap, counts, cap, tab_v)
    to_scalars = pltpu.make_async_copy(tab_v, tab, loc.at[6])
    to_scalars.start()

    loads[2].wait()
    tiles = a_v.shape[1] // 128

    def turn(i):
        at_v[pl.ds(i * 128, 128), :] = a_v[:, pl.ds(pl.multiple_of(i * 128, 128), 128)].T

    loop(0, tiles, turn)
    loads[3].wait()
    wide = 256
    per = width // wide

    def multiply(n):
        got = jnp.dot(
            at_v[...],
            c_v[:, pl.ds(pl.multiple_of(n * wide, wide), wide)],
            preferred_element_type=f32,
        )
        got = got.astype(bf16).reshape(part.shape[0], rows, wide)
        part[:, n // per, :, pl.ds(pl.multiple_of((n % per) * wide, wide), wide)] = got

    loop(0, c_v.shape[1] // wide, multiply)
    ncol = c_v.shape[1] // width
    to_scalars.wait()

    def arrange(s):
        b = tab[2, s]
        q[s % COLS, s // COLS] = part[b // ncol, b % ncol]

    loop(0, COLS * nz, arrange)

    loads[0].wait()
    loads[1].wait()
    start_me = tab[1, dp]

    def slot_for(col):
        return (col + 4 * COLS * nz - start_me) % COLS

    for k in range(COLS):
        r = slot_for((x + k) % COLS)
        rxs[0, k] = lr_v[r]
        rxs[1, k] = rr_v[r]
    rx_l[x] = rxs[0, 0]
    rx_r[x] = rxs[1, 0]

    def root_x(which, k):
        return send(
            rxs.at[which, k], rx[which].at[x], s_rx.at[which, k], r_rx.at[which, k], at_x(k)
        )

    def root_z(which, k):
        return send(
            rzs.at[which, (z + k) % nz],
            rz[which].at[z],
            s_rz.at[which, k - 1],
            r_rz.at[which, k - 1],
            at_z(k),
        )

    def root_turn(which):
        for k in range(1, COLS):
            root_x(which, k).wait_recv()

        def root_row(k):
            row = (z + k) % nz
            rzs[which, row] = rx[which][tab[3, row * COLS + x] % COLS]

        loop(0, nz, root_row)
        rz[which][z] = rzs[which, z]
        loop(1, nz, lambda k: root_z(which, k).start())

    pl.semaphore_wait(barrier, COLS - 1 + nz - 1 + mp - 1)
    lo, hi = pl.ds(0, half), pl.ds(half, half)
    far, right, left = (x + 2) % COLS, (x + 1) % COLS, (x + 3) % COLS

    def x_copy(h, j, src, dst, k):
        return send(
            src.at[:, part_rows[h], :],
            dst.at[:, part_rows[h], :],
            s_x.at[h, j],
            r_x.at[h, j],
            at_x(k),
        )

    relay, direct, onward = [], [], []
    for h in range(2):
        relay.append(
            [
                x_copy(h, 0, q.at[far, lo], rel.at[0], 1),
                x_copy(h, 1, q.at[far, hi], rel.at[1], 3),
            ]
        )
        direct.append(
            [
                x_copy(h, 2, q.at[right, hi], xa.at[0], 1),
                x_copy(h, 3, q.at[left, lo], xa.at[1], 3),
            ]
        )
        onward.append(
            [x_copy(h, 4, fwd.at[0], xa.at[2], 1), x_copy(h, 5, fwd.at[1], xa.at[3], 3)]
        )
    for k in range(1, COLS):
        root_x(1, k).start()
    for copy in relay[0] + direct[0] + relay[1]:
        copy.start()

    def send_on(h):
        at = part_rows[h]
        for side, (toward, part_of) in enumerate([(right, lo), (left, hi)]):
            relay[h][side].wait_recv()
            fwd[side, :, at, :] = (
                q[toward, part_of, at, :].astype(f32) + rel[side, :, at, :].astype(f32)
            ).astype(bf16)
            onward[h][side].start()

    send_on(0)
    for copy in direct[1]:
        copy.start()
    root_turn(1)
    send_on(1)
    for k in range(1, COLS):
        root_x(0, k).start()

    def z_send(h, k):
        return send(
            xsum.at[(z + k) % nz, part_rows[h], :],
            zr.at[k - 1, part_rows[h], :],
            s_z.at[h, k - 1],
            r_z.at[h, k - 1],
            at_z(k),
        )

    def z_copy(h, way, kind):
        def there(k):
            return k if way == 0 else nz - k

        at = part_rows[h]
        cols = pl.ds(way * (width // 2), width // 2)
        j = 4 * way + kind
        if kind == 0:
            src, dst, k = xsum.at[(z + there(1)) % nz, at, :], zr.at[way, at, :], 1
        elif kind == 1:
            src, dst, k = xsum.at[(z + there(3)) % nz, at, :], zrel.at[way, 0, at, :], 1
        elif kind == 2:
            src, dst, k = xsum.at[(z + there(4)) % nz, at, cols], zrel.at[way, 1, at, cols], 2
        else:
            src, dst, k = zfwd.at[way, at, :], zr.at[2 + way, at, :], 2
        return send(src, dst, s_z.at[h, j], r_z.at[h, j], at_z(there(k)))

    def z_start(h):
        if nz != 8:
            loop(1, nz, lambda k: z_send(h, k).start())
            return
        for kind in (2, 1, 0):
            for way in range(2):
                z_copy(h, way, kind).start()

    def z_onward(h):
        if nz != 8:
            return
        at = part_rows[h]
        for way in range(2):
            cols = pl.ds(way * (width // 2), width // 2)
            z_copy(h, way, 1).wait_recv()
            z_copy(h, way, 2).wait_recv()
            to = (z + (2 if way == 0 else nz - 2)) % nz
            both = xsum[to, at, :].astype(f32) + zrel[way, 0, at, :].astype(f32)
            extra = zrel[way, 1, at, cols].astype(f32)
            none = jnp.zeros_like(extra)
            extra = jnp.concatenate([extra, none] if way == 0 else [none, extra], axis=1)
            zfwd[way, at, :] = (both + extra).astype(bf16)
            z_copy(h, way, 3).start()

    def z_finish(h):
        at = part_rows[h]
        total = xsum[z, at, :].astype(f32)
        if nz != 8:
            loop(1, nz, lambda k: z_send(h, k).wait_recv())
            for k in range(nz - 1):
                total = total + zr[k, at, :].astype(f32)
            return total
        for way in range(2):
            z_copy(h, way, 0).wait_recv()
            z_copy(h, way, 3).wait_recv()
            total = total + zr[way, at, :].astype(f32) + zr[2 + way, at, :].astype(f32)
        return total

    def z_drain(h):
        if nz != 8:
            loop(1, nz, lambda k: z_send(h, k).wait_send())
            return
        for way in range(2):
            for kind in range(4):
                z_copy(h, way, kind).wait_send()

    def x_done(h):
        at = part_rows[h]
        for copy in direct[h] + onward[h]:
            copy.wait_recv()
        own = q[x, :, at, :].astype(f32)
        xsum[lo, at, :] = (
            own[:half] + xa[1, :, at, :].astype(f32) + xa[2, :, at, :].astype(f32)
        ).astype(bf16)
        xsum[hi, at, :] = (
            own[half:] + xa[0, :, at, :].astype(f32) + xa[3, :, at, :].astype(f32)
        ).astype(bf16)
        z_start(h)

    x_done(0)
    x_done(1)

    z_onward(0)
    loop(1, nz, lambda k: root_z(1, k).wait_recv())
    source = tab[3, dp] // COLS
    rful[m] = rz_r[source]

    def over_mp(full, j, at):
        def ref(origin, side):
            cols = slice(None) if side is None else pl.ds(side * (width // 2), width // 2)
            return full.at[origin * 2 + c, at, cols]

        def across(k):
            r = ref((y + ny - k) % ny, None)
            return send(r, r, s_c.at[j, k], r_c.at[j, k], partner)

        return spread(y, ny, at_y, ref, s_y.at[j], r_y.at[j]), across

    (r_start, r_forward, r_finish, r_drain), r_across = over_mp(rful, 2, pl.ds(0, rows))
    g_over = [over_mp(gful, h, part_rows[h]) for h in range(2)]
    r_start(0)
    r_across(0).start()
    z_onward(1)
    root_turn(0)

    def z_done(h):
        gful[m, part_rows[h], :] = z_finish(h).astype(bf16)
        (start, _, _, _), across = g_over[h]
        start(0)
        across(0).start()

    z_done(0)
    r_forward()
    z_done(1)
    g_over[0][0][1]()
    r_finish(lambda k: r_across(k).start())
    g_over[1][0][1]()
    for h in range(2):
        (_, _, finish, _), across = g_over[h]
        finish(lambda k, across=across: across(k).start())
    for _, across in g_over:
        loop(0, ny, lambda k, across=across: across(k).wait_recv())
    loop(0, ny, lambda k: r_across(k).wait_recv())
    loop(1, nz, lambda k: root_z(0, k).wait_recv())

    order = mp * rows
    g = gful[...].reshape(order, width)
    applied = jnp.dot(rz_l[source], g, preferred_element_type=f32).astype(bf16)
    cond = jnp.dot(applied, rful[...].reshape(order, width), preferred_element_type=f32)
    cond_v[...] = cond
    partial_sum = jnp.broadcast_to(jnp.sum(cond * cond, keepdims=True), ssq_s.shape)
    ssq_s[...] = partial_sum
    ssq[m] = partial_sum

    def square_send(k):
        return send(ssq_s, ssq.at[m], s_q.at[k - 1], r_q.at[k - 1], at_m(k))

    loop(1, mp, lambda k: square_send(k).start())

    z_over = [
        spread(z, nz, at_z, lambda o, side, b=b: b.at[o] if side is None else b.at[o, :, pl.ds(side * (width // 2), width // 2)], s_f.at[i], r_f.at[i])
        for i, b in enumerate(zb)
    ]

    mine = gful[m]
    zb_l[z] = lax.dot_general(
        mine, g, (((1,), (1,)), ((), ())), preferred_element_type=f32
    ).astype(bf16)
    z_over[0][0](0)
    piece = pl.multiple_of((m * rows // 128) * 128, 128)
    columns = gful[:, :, pl.ds(piece, 128)].reshape(order, 128)
    slab[...] = lax.dot_general(columns, g, (((0,), (0,)), ((), ())), preferred_element_type=f32)
    zb_r[z] = slab[pl.ds((m * rows) % 128, rows), :].astype(bf16)
    z_over[1][0](0)
    wide_g = g.astype(f32)
    grad_square = jnp.sum(wide_g * wide_g, keepdims=True)
    loads[4].start()
    loads[5].start()
    z_over[0][1]()
    loop(1, mp, lambda k: square_send(k).wait_recv())
    cond_square = jnp.sum(ssq[...], axis=0)[0:1, 0:1]
    entries = float(order * width)
    ratio = jnp.sqrt((grad_square / entries + epsilon) / (cond_square / entries + epsilon))
    zb_u[z] = (cond_v[...] * ratio).astype(bf16)
    z_over[2][0](0)
    z_over[1][1]()
    z_over[2][1]()
    z_over[0][2]()
    z_over[1][2]()

    def pick(col, place):
        begin = tab[1, z * COLS + col]
        k = (begin + (x + 4 * COLS * nz - begin) % COLS) // COLS
        k = jnp.minimum(k, nz - 1)
        place[0] = zb_l[k]
        place[1] = zb_r[k]

    def fin(j, k):
        src = fxs.at[k - 1] if j == 0 else fxs_u.at[k - 1]
        dst = fx.at[x] if j == 0 else fx_u.at[x]
        return send(src, dst, s_fx.at[j, k - 1], r_fx.at[j, k - 1], at_x(k))

    def pick_update(col):
        return zb_u[tab[0, z * COLS + col] // COLS]

    for k in (2, 1, 3):
        pick((x + k) % COLS, fxs.at[k - 1])
        fin(0, k).start()
    pick(x, fx.at[x])
    z_over[2][2]()
    for k in (2, 1, 3):
        fxs_u[k - 1] = pick_update((x + k) % COLS)
        fin(1, k).start()
    fx_u[x] = pick_update(x)
    for h in range(2):
        for copy in relay[h] + direct[h] + onward[h]:
            copy.wait_send()
        z_drain(h)
        g_over[h][0][3]()
        loop(0, ny, lambda k, h=h: g_over[h][1](k).wait_send())
        loop(1, nz, lambda k, h=h: root_z(h, k).wait_send())
        for k in range(1, COLS):
            root_x(h, k).wait_send()
    r_drain()
    loop(0, ny, lambda k: r_across(k).wait_send())
    loop(1, mp, lambda k: square_send(k).wait_send())
    for over in z_over:
        over[3]()
    for k in range(1, COLS):
        fin(0, k).wait_recv()
    loads[4].wait()
    loads[5].wait()
    limit = tab[4, dp]
    for r in range(cap):
        col = (start_me + r) % COLS
        live = limit > r
        new_left[r] = ls_v[r] + jnp.where(live, fx[col, 0].astype(f32), 0.0)
        new_right[r] = rs_v[r] + jnp.where(live, fx[col, 1].astype(f32), 0.0)
    for k in range(1, COLS):
        fin(1, k).wait_recv()
    home = fx_u[tab[0, dp] % COLS].astype(f32)
    upd[0] = jnp.where(tab[5, dp] > 0, home, 0.0).astype(bf16)
    for j in range(2):
        for k in range(1, COLS):
            fin(j, k).wait_send()


def tables(omap, counts, capacity, out):
    blocks = omap.shape[1]
    shape = (blocks, blocks)
    i = lax.broadcasted_iota(jnp.int32, shape, 0)
    j = lax.broadcasted_iota(jnp.int32, shape, 1)

    def over_i(value):
        return jnp.sum(value.astype(jnp.int32), axis=0, keepdims=True)

    def over_j(value):
        return jnp.sum(value.astype(jnp.int32), axis=1, keepdims=True)

    row = jnp.broadcast_to(omap[...], shape)
    many = jnp.broadcast_to(counts[...], shape)
    col = jnp.broadcast_to(over_j(jnp.where(i == j, row, 0)), shape)
    many_col = jnp.broadcast_to(over_j(jnp.where(i == j, many, 0)), shape)
    rank = over_i(jnp.where((col == row) & (i < j), 1, 0))
    place = over_i(jnp.where(col < row, 1, 0)) + rank
    place_col = over_j(jnp.where((row < col) | ((row == col) & (j < i)), 1, 0))
    at = jnp.broadcast_to(place_col, shape) == j
    limit = jnp.minimum(over_i(jnp.where(col == j, 1, 0)), counts[...])
    held = over_i(jnp.where(row == i, many_col, 0))
    live = jnp.where((rank < held) & (rank < capacity), 1, 0)
    for n, value in enumerate(
        [
            place,
            over_i(jnp.where(col < j, 1, 0)),
            over_i(jnp.where(at, i, 0)),
            over_i(jnp.where(at, col, 0)),
            jnp.minimum(limit, capacity),
            live,
        ]
    ):
        out[n : n + 1, 0:blocks] = value


def shards(acts, cot, lstat, rstat, lroot, rroot, owner_map, owner_counts):
    cap, rows, width = lstat.shape
    tok, own = acts.shape
    dw = cot.shape[1]
    devices, mp = lax.axis_size("dp"), lax.axis_size("mp")
    nz, ny = devices // COLS, mp // 2
    sizes = (nz, ny, mp, rows, width, cap)
    V, D = pltpu.VMEM, pltpu.SemaphoreType.DMA
    half = nz // 2

    def pieces(*lead):
        return V((*lead, rows, width), bf16)

    scratch = [
        V((8, 128), jnp.int32),
        pltpu.SMEM((8, 128), jnp.int32),
        V((tok, own), bf16),
        V((own, tok), bf16),
        V((tok, dw), bf16),
        V(lstat.shape, f32),
        V(rstat.shape, f32),
        V(lroot.shape, bf16),
        V(rroot.shape, bf16),
        pieces(own // rows, dw // width),
        pieces(COLS, nz),
        pieces(2, half),
        pieces(4, half),
        pieces(2, half),
        pieces(nz),
        pieces(max(nz - 1, 4)),
        pieces(mp),
        pieces(mp),
        pieces(2, COLS),
        pieces(COLS),
        pieces(COLS),
        pieces(2, nz),
        pieces(nz),
        pieces(nz),
        pieces(2, 2),
        pieces(2),
        V((128, width), f32),
        V((rows, width), f32),
        V((8, 128), f32),
        V((mp, 8, 128), f32),
        pieces(nz),
        pieces(nz),
        pieces(nz),
        pieces(COLS - 1, 2),
        pieces(COLS - 1),
        pieces(COLS, 2),
        pieces(COLS),
        D((7,)),
    ]
    for shape in [
        (2, COLS),
        (2, nz - 1),
        (2, 6),
        (2, max(nz - 1, 8)),
        (3, 2, 4),
        (3, ny),
        (mp - 1,),
        (3, 2, 4),
        (2, COLS - 1),
    ]:
        scratch += [D(shape), D(shape)]
    anywhere = pl.BlockSpec(memory_space=pl.ANY)
    vmem = pl.BlockSpec(memory_space=pltpu.VMEM)
    return pl.pallas_call(
        functools.partial(kernel, sizes),
        out_shape=(
            jax.ShapeDtypeStruct((1, rows, width), bf16),
            jax.ShapeDtypeStruct(lstat.shape, f32),
            jax.ShapeDtypeStruct(rstat.shape, f32),
        ),
        in_specs=[vmem] * 2 + [anywhere] * 6,
        out_specs=(vmem,) * 3,
        scratch_shapes=scratch,
        compiler_params=pltpu.CompilerParams(collective_id=0, has_side_effects=True),
        name="shampoo",
    )(owner_map[None], owner_counts[None], acts, cot, lstat, rstat, lroot, rroot)


def solution(mesh):
    in_specs = (
        P("dp", "mp"),
        P("dp", None),
        P("dp", "mp", None),
        P("dp", "mp", None),
        P("dp", "mp", None),
        P("dp", "mp", None),
        P(),
        P(),
    )
    out_specs = (P("dp", "mp", None), P("dp", "mp", None), P("dp", "mp", None))
    return jax.shard_map(shards, mesh=mesh, in_specs=in_specs, out_specs=out_specs, check_vma=False)
```

```python
import functools

import jax
import jax.numpy as jnp
from jax import lax
from jax.experimental import pallas as pl
from jax.experimental.pallas import tpu as pltpu
from jax.sharding import PartitionSpec as P

epsilon = 1e-06
COLS = 4
MESH = pl.DeviceIdType.MESH
PLANS = {
    1: (),
    2: ((0, 0, 1, False),),
    4: ((0, 0, 1, True), (0, 0, 2, False)),
    8: ((0, 0, 1, True), (0, 0, 2, True), (1, 2, 1, True), (1, 2, 2, False)),
}
f32, bf16 = jnp.float32, jnp.bfloat16


def kernel(
    sizes,
    omap,
    counts,
    acts,
    cot,
    lroot,
    rroot,
    result,
    om_v,
    ct_v,
    tab_v,
    tab,
    a_v,
    at_v,
    c_v,
    lr_v,
    rr_v,
    part,
    q,
    rel,
    xa,
    fwd,
    xsum,
    zr,
    gful,
    rful,
    rxs,
    rx_l,
    rx_r,
    rzs,
    rz_l,
    rz_r,
    zrel,
    zfwd,
    slab,
    cond_v,
    ssq_s,
    ssq,
    zb_l,
    zb_r,
    zb_u,
    fxs,
    fx_l,
    fx_r,
    fx_u,
    packed,
    loc,
    s_rx,
    r_rx,
    s_rz,
    r_rz,
    s_x,
    r_x,
    s_z,
    r_z,
    s_y,
    r_y,
    s_c,
    r_c,
    s_q,
    r_q,
    s_f,
    r_f,
    s_fx,
    r_fx,
):
    nz, ny, mp, rows, width, cap = sizes
    dp = lax.axis_index("dp")
    m = lax.axis_index("mp")
    x, z = dp % COLS, dp // COLS
    c, y = m % 2, m // 2
    half = nz // 2
    rx, rz, zb = (rx_l, rx_r), (rz_l, rz_r), (zb_l, zb_r, zb_u)
    fx = (fx_l, fx_r, fx_u)
    part_rows = [pl.ds(h * (rows // 2), rows // 2) for h in range(2)]

    def at_x(k):
        return {"dp": z * COLS + (x + k) % COLS}

    def at_z(k):
        return {"dp": ((z + k) % nz) * COLS + x}

    def at_y(k):
        return {"mp": ((y + k) % ny) * 2 + c}

    def at_m(k):
        return {"mp": (m + k) % mp}

    partner = {"mp": y * 2 + (1 - c)}

    def send(src, dst, ssem, rsem, where):
        return pltpu.make_async_remote_copy(
            src_ref=src,
            dst_ref=dst,
            send_sem=ssem,
            recv_sem=rsem,
            device_id=where,
            device_id_type=MESH,
        )

    def loop(lo, hi, body):
        def step(i, carry):
            body(i)
            return carry

        lax.fori_loop(lo, hi, step, 0)

    def spread(pos, n, where, ref, ssem, rsem):
        plan = PLANS[n]

        def copy(i, way):
            _, behind, hop, whole = plan[i]
            origin = (pos + n - behind) % n if way == 0 else (pos + behind) % n
            r = ref(origin, None if whole else way)
            return send(
                r, r, ssem.at[way, i], rsem.at[way, i], where(hop if way == 0 else n - hop)
            )

        def start(stage):
            for i, item in enumerate(plan):
                if item[0] == stage:
                    for way in range(2):
                        copy(i, way).start()

        def forward():
            if len(plan) > 2:
                for way in range(2):
                    copy(1, way).wait_recv()
                start(1)

        def finish(arrived=None):
            for i, item in enumerate(plan):
                for way in range(2):
                    if not (len(plan) > 2 and i == 1):
                        copy(i, way).wait_recv()
                if arrived is not None:
                    far = item[1] + item[2]
                    arrived(far)
                    if item[3]:
                        arrived(n - far)

        def drain():
            for i in range(len(plan)):
                for way in range(2):
                    copy(i, way).wait_send()

        return start, forward, finish, drain

    barrier = pltpu.get_barrier_semaphore()

    def hello(where):
        pl.semaphore_signal(barrier, inc=1, device_id=where, device_id_type=MESH)

    loads = [
        pltpu.make_async_copy(s, d, loc.at[i])
        for i, (s, d) in enumerate(
            [
                (lroot, lr_v),
                (rroot, rr_v),
                (acts, a_v),
                (cot, c_v),
                (omap, om_v),
                (counts, ct_v),
            ]
        )
    ]
    for i in (4, 5, 2, 3, 1, 0):
        loads[i].start()
    for k in range(1, COLS):
        hello(at_x(k))
    loop(1, nz, lambda k: hello(at_z(k)))
    loop(1, mp, lambda k: hello(at_m(k)))

    loads[4].wait()
    loads[5].wait()
    tables(om_v, ct_v, cap, tab_v)
    to_scalars = pltpu.make_async_copy(tab_v, tab, loc.at[6])
    to_scalars.start()

    loads[2].wait()
    tiles = a_v.shape[1] // 128
    each = 128 // rows

    def turn(i):
        columns = a_v[:, pl.ds(pl.multiple_of(i * 128, 128), 128)]
        at_v[pl.ds(i * each, each)] = columns.T.reshape(each, rows, a_v.shape[0])

    loop(0, tiles, turn)
    to_scalars.wait()
    loads[0].wait()
    loads[1].wait()
    start_me = tab[1, dp]

    def slot_for(col):
        return (col + 4 * COLS * nz - start_me) % COLS

    for k in range(COLS):
        r = slot_for((x + k) % COLS)
        rxs[0, k] = lr_v[r]
        rxs[1, k] = rr_v[r]
    rx_l[x] = rxs[0, 0]
    rx_r[x] = rxs[1, 0]

    def root_x(which, k):
        return send(
            rxs.at[which, k], rx[which].at[x], s_rx.at[which, k], r_rx.at[which, k], at_x(k)
        )

    def root_z(which, k):
        return send(
            rzs.at[which, (z + k) % nz],
            rz[which].at[z],
            s_rz.at[which, k - 1],
            r_rz.at[which, k - 1],
            at_z(k),
        )

    def root_turn(which):
        for k in range(1, COLS):
            root_x(which, k).wait_recv()

        def root_row(k):
            row = (z + k) % nz
            rzs[which, row] = rx[which][tab[3, row * COLS + x] % COLS]

        loop(0, nz, root_row)
        rz[which][z] = rzs[which, z]
        loop(1, nz, lambda k: root_z(which, k).start())

    pl.semaphore_wait(barrier, COLS - 1 + nz - 1 + mp - 1)
    for k in (2, 1, 3):
        root_x(1, k).start()
    loads[3].wait()

    wide = 256
    per = width // wide
    ncol = c_v.shape[1] // width

    def multiply(n):
        got = jnp.dot(
            at_v[...].reshape(-1, c_v.shape[0]),
            c_v[:, pl.ds(pl.multiple_of(n * wide, wide), wide)],
            preferred_element_type=f32,
        )
        got = got.astype(bf16).reshape(part.shape[0], rows, wide)
        part[:, n // per, :, pl.ds(pl.multiple_of((n % per) * wide, wide), wide)] = got

    def arrange(h):
        at = part_rows[h]

        def one(s):
            b = tab[2, s]
            q[s % COLS, s // COLS, at, :] = part[b // ncol, b % ncol, at, :]

        loop(0, COLS * nz, one)

    loop(0, c_v.shape[1] // wide, multiply)
    arrange(0)
    lo, hi = pl.ds(0, half), pl.ds(half, half)
    far, right, left = (x + 2) % COLS, (x + 1) % COLS, (x + 3) % COLS

    def x_copy(h, j, src, dst, k):
        return send(
            src.at[:, part_rows[h], :],
            dst.at[:, part_rows[h], :],
            s_x.at[h, j],
            r_x.at[h, j],
            at_x(k),
        )

    relay, direct, onward = [], [], []
    for h in range(2):
        relay.append(
            [
                x_copy(h, 0, q.at[far, lo], rel.at[0], 1),
                x_copy(h, 1, q.at[far, hi], rel.at[1], 3),
            ]
        )
        direct.append(
            [
                x_copy(h, 2, q.at[right, hi], xa.at[0], 1),
                x_copy(h, 3, q.at[left, lo], xa.at[1], 3),
            ]
        )
        onward.append(
            [x_copy(h, 4, fwd.at[0], xa.at[2], 1), x_copy(h, 5, fwd.at[1], xa.at[3], 3)]
        )
    for copy in relay[0] + direct[0]:
        copy.start()
    arrange(1)
    for copy in relay[1]:
        copy.start()

    def send_on(h):
        at = part_rows[h]
        for side, (toward, part_of) in enumerate([(right, lo), (left, hi)]):
            relay[h][side].wait_recv()
            fwd[side, :, at, :] = (
                q[toward, part_of, at, :].astype(f32) + rel[side, :, at, :].astype(f32)
            ).astype(bf16)
            onward[h][side].start()

    send_on(0)
    for copy in direct[1]:
        copy.start()
    root_turn(1)
    send_on(1)
    for k in range(1, COLS):
        root_x(0, k).start()

    def z_send(h, k):
        return send(
            xsum.at[(z + k) % nz, part_rows[h], :],
            zr.at[k - 1, part_rows[h], :],
            s_z.at[h, k - 1],
            r_z.at[h, k - 1],
            at_z(k),
        )

    def z_copy(h, way, kind):
        def there(k):
            return k if way == 0 else nz - k

        at = part_rows[h]
        cols = pl.ds(way * (width // 2), width // 2)
        j = 4 * way + kind
        if kind == 0:
            src, dst, k = xsum.at[(z + there(1)) % nz, at, :], zr.at[way, at, :], 1
        elif kind == 1:
            src, dst, k = xsum.at[(z + there(3)) % nz, at, :], zrel.at[way, 0, at, :], 1
        elif kind == 2:
            src, dst, k = xsum.at[(z + there(4)) % nz, at, cols], zrel.at[way, 1, at, cols], 2
        else:
            src, dst, k = zfwd.at[way, at, :], zr.at[2 + way, at, :], 2
        return send(src, dst, s_z.at[h, j], r_z.at[h, j], at_z(there(k)))

    def z_start(h):
        if nz != 8:
            loop(1, nz, lambda k: z_send(h, k).start())
            return
        for kind in (2, 1, 0):
            for way in range(2):
                z_copy(h, way, kind).start()

    def z_onward(h):
        if nz != 8:
            return
        at = part_rows[h]
        for way in range(2):
            cols = pl.ds(way * (width // 2), width // 2)
            z_copy(h, way, 1).wait_recv()
            z_copy(h, way, 2).wait_recv()
            to = (z + (2 if way == 0 else nz - 2)) % nz
            both = xsum[to, at, :].astype(f32) + zrel[way, 0, at, :].astype(f32)
            extra = zrel[way, 1, at, cols].astype(f32)
            none = jnp.zeros_like(extra)
            extra = jnp.concatenate([extra, none] if way == 0 else [none, extra], axis=1)
            zfwd[way, at, :] = (both + extra).astype(bf16)
            z_copy(h, way, 3).start()

    def z_finish(h):
        at = part_rows[h]
        total = xsum[z, at, :].astype(f32)
        if nz != 8:
            loop(1, nz, lambda k: z_send(h, k).wait_recv())
            for k in range(nz - 1):
                total = total + zr[k, at, :].astype(f32)
            return total
        for way in range(2):
            z_copy(h, way, 0).wait_recv()
            z_copy(h, way, 3).wait_recv()
            total = total + zr[way, at, :].astype(f32) + zr[2 + way, at, :].astype(f32)
        return total

    def z_drain(h):
        if nz != 8:
            loop(1, nz, lambda k: z_send(h, k).wait_send())
            return
        for way in range(2):
            for kind in range(4):
                z_copy(h, way, kind).wait_send()

    def x_done(h):
        at = part_rows[h]
        for copy in direct[h] + onward[h]:
            copy.wait_recv()
        own = q[x, :, at, :].astype(f32)
        xsum[lo, at, :] = (
            own[:half] + xa[1, :, at, :].astype(f32) + xa[2, :, at, :].astype(f32)
        ).astype(bf16)
        xsum[hi, at, :] = (
            own[half:] + xa[0, :, at, :].astype(f32) + xa[3, :, at, :].astype(f32)
        ).astype(bf16)
        z_start(h)

    x_done(0)
    x_done(1)

    z_onward(0)
    loop(1, nz, lambda k: root_z(1, k).wait_recv())
    source = tab[3, dp] // COLS
    rful[m] = rz_r[source]

    def over_mp(full, j, at):
        def ref(origin, side):
            cols = slice(None) if side is None else pl.ds(side * (width // 2), width // 2)
            return full.at[origin * 2 + c, at, cols]

        def across(k):
            r = ref((y + ny - k) % ny, None)
            return send(r, r, s_c.at[j, k], r_c.at[j, k], partner)

        return spread(y, ny, at_y, ref, s_y.at[j], r_y.at[j]), across

    (r_start, r_forward, r_finish, r_drain), r_across = over_mp(rful, 2, pl.ds(0, rows))
    g_over = [over_mp(gful, h, part_rows[h]) for h in range(2)]
    r_start(0)
    r_across(0).start()
    z_onward(1)
    root_turn(0)

    def z_done(h):
        gful[m, part_rows[h], :] = z_finish(h).astype(bf16)
        (start, _, _, _), across = g_over[h]
        start(0)
        across(0).start()

    z_done(0)
    r_forward()
    z_done(1)
    g_over[0][0][1]()
    g_over[1][0][1]()
    r_finish(lambda k: r_across(k).start())
    for h in range(2):
        (_, _, finish, _), across = g_over[h]
        finish(lambda k, across=across: across(k).start())
    for _, across in g_over:
        loop(0, ny, lambda k, across=across: across(k).wait_recv())
    loop(0, ny, lambda k: r_across(k).wait_recv())
    loop(1, nz, lambda k: root_z(0, k).wait_recv())

    order = mp * rows
    g = gful[...].reshape(order, width)
    applied = jnp.dot(rz_l[source], g, preferred_element_type=f32).astype(bf16)
    cond = jnp.dot(applied, rful[...].reshape(order, width), preferred_element_type=f32)
    cond_v[...] = cond
    partial_sum = jnp.broadcast_to(jnp.sum(cond * cond, keepdims=True), ssq_s.shape)
    ssq_s[...] = partial_sum
    ssq[m] = partial_sum

    def square_send(k):
        return send(ssq_s, ssq.at[m], s_q.at[k - 1], r_q.at[k - 1], at_m(k))

    loop(1, mp, lambda k: square_send(k).start())

    z_over = [
        spread(z, nz, at_z, lambda o, side, b=b: b.at[o] if side is None else b.at[o, :, pl.ds(side * (width // 2), width // 2)], s_f.at[i], r_f.at[i])
        for i, b in enumerate(zb)
    ]

    mine = gful[m]
    zb_l[z] = lax.dot_general(
        mine, g, (((1,), (1,)), ((), ())), preferred_element_type=f32
    ).astype(bf16)
    z_over[0][0](0)
    piece = pl.multiple_of((m * rows // 128) * 128, 128)
    columns = gful[:, :, pl.ds(piece, 128)].reshape(order, 128)
    slab[...] = lax.dot_general(columns, g, (((0,), (0,)), ((), ())), preferred_element_type=f32)
    zb_r[z] = slab[pl.ds((m * rows) % 128, rows), :].astype(bf16)
    z_over[1][0](0)
    wide_g = g.astype(f32)
    grad_square = jnp.sum(wide_g * wide_g, keepdims=True)
    z_over[0][1]()
    loop(1, mp, lambda k: square_send(k).wait_recv())
    cond_square = jnp.sum(ssq[...], axis=0)[0:1, 0:1]
    entries = float(order * width)
    ratio = jnp.sqrt((grad_square / entries + epsilon) / (cond_square / entries + epsilon))
    zb_u[z] = (cond_v[...] * ratio).astype(bf16)
    z_over[2][0](0)
    z_over[1][1]()

    def seat_row(col):
        begin = tab[1, z * COLS + col]
        k = (begin + (x + 4 * COLS * nz - begin) % COLS) // COLS
        return jnp.minimum(k, nz - 1)

    def fin(j, k):
        return send(
            fxs.at[j, k - 1], fx[j].at[x], s_fx.at[j, k - 1], r_fx.at[j, k - 1], at_x(k)
        )

    def go_on(j):
        def pick(col):
            return zb[j][seat_row(col) if j < 2 else tab[0, z * COLS + col] // COLS]

        for k in (2, 1, 3):
            fxs[j, k - 1] = pick((x + k) % COLS)
            fin(j, k).start()
        fx[j][x] = pick(x)

    z_over[0][2]()
    go_on(0)
    z_over[2][1]()
    z_over[1][2]()
    go_on(1)
    z_over[2][2]()
    go_on(2)
    for h in range(2):
        for copy in relay[h] + direct[h] + onward[h]:
            copy.wait_send()
        z_drain(h)
        g_over[h][0][3]()
        loop(0, ny, lambda k, h=h: g_over[h][1](k).wait_send())
        loop(1, nz, lambda k, h=h: root_z(h, k).wait_send())
        for k in range(1, COLS):
            root_x(h, k).wait_send()
    r_drain()
    loop(0, ny, lambda k: r_across(k).wait_send())
    loop(1, mp, lambda k: square_send(k).wait_send())
    for over in z_over:
        over[3]()
    limit = tab[4, dp]

    def put(j):
        at = pl.ds(j * cap, cap if j < 2 else 1)
        return pltpu.make_async_copy(packed.at[at], result.at[at], loc.at[7 + j])

    for j in range(2):
        for k in range(1, COLS):
            fin(j, k).wait_recv()
        for r in range(cap):
            add = fx[j][(start_me + r) % COLS]
            packed[j * cap + r] = jnp.where(limit > r, add, jnp.zeros_like(add))
        put(j).start()
    for k in range(1, COLS):
        fin(2, k).wait_recv()
    home = fx[2][tab[0, dp] % COLS]
    packed[2 * cap] = jnp.where(tab[5, dp] > 0, home, jnp.zeros_like(home))
    put(2).start()
    for j in range(3):
        for k in range(1, COLS):
            fin(j, k).wait_send()
    for j in range(3):
        put(j).wait()


def finish(result, lstat, rstat, upd, new_left, new_right, packed, old, new, loc, out):
    cap = old.shape[1]
    get = [
        pltpu.make_async_copy(s, d, loc.at[i])
        for i, (s, d) in enumerate([(result, packed), (lstat, old.at[0]), (rstat, old.at[1])])
    ]
    for copy in get:
        copy.start()
    get[0].wait()
    put = [pltpu.make_async_copy(packed.at[pl.ds(2 * cap, 1)], upd, out.at[0])]
    put[0].start()
    for j, to in enumerate([new_left, new_right]):
        get[1 + j].wait()
        new[j] = old[j] + packed[pl.ds(j * cap, cap)].astype(f32)
        copy = pltpu.make_async_copy(new.at[j], to, out.at[1 + j])
        copy.start()
        put.append(copy)
    for copy in put:
        copy.wait()


def tables(omap, counts, capacity, out):
    blocks = omap.shape[1]
    shape = (blocks, blocks)
    i = lax.broadcasted_iota(jnp.int32, shape, 0)
    j = lax.broadcasted_iota(jnp.int32, shape, 1)

    def over_i(value):
        return jnp.sum(value.astype(jnp.int32), axis=0, keepdims=True)

    def over_j(value):
        return jnp.sum(value.astype(jnp.int32), axis=1, keepdims=True)

    row = jnp.broadcast_to(omap[...], shape)
    many = jnp.broadcast_to(counts[...], shape)
    col = jnp.broadcast_to(over_j(jnp.where(i == j, row, 0)), shape)
    many_col = jnp.broadcast_to(over_j(jnp.where(i == j, many, 0)), shape)
    rank = over_i(jnp.where((col == row) & (i < j), 1, 0))
    place = over_i(jnp.where(col < row, 1, 0)) + rank
    place_col = over_j(jnp.where((row < col) | ((row == col) & (j < i)), 1, 0))
    at = jnp.broadcast_to(place_col, shape) == j
    limit = jnp.minimum(over_i(jnp.where(col == j, 1, 0)), counts[...])
    held = over_i(jnp.where(row == i, many_col, 0))
    live = jnp.where((rank < held) & (rank < capacity), 1, 0)
    for n, value in enumerate(
        [
            place,
            over_i(jnp.where(col < j, 1, 0)),
            over_i(jnp.where(at, i, 0)),
            over_i(jnp.where(at, col, 0)),
            jnp.minimum(limit, capacity),
            live,
        ]
    ):
        out[n : n + 1, 0:blocks] = value


def shards(acts, cot, lstat, rstat, lroot, rroot, owner_map, owner_counts):
    cap, rows, width = lstat.shape
    tok, own = acts.shape
    dw = cot.shape[1]
    devices, mp = lax.axis_size("dp"), lax.axis_size("mp")
    nz, ny = devices // COLS, mp // 2
    sizes = (nz, ny, mp, rows, width, cap)
    V, D = pltpu.VMEM, pltpu.SemaphoreType.DMA
    half = nz // 2

    def pieces(*lead):
        return V((*lead, rows, width), bf16)

    scratch = [
        V((1, devices), jnp.int32),
        V((1, devices), jnp.int32),
        V((8, 128), jnp.int32),
        pltpu.SMEM((8, 128), jnp.int32),
        V((tok, own), bf16),
        V((own // rows, rows, tok), bf16),
        V((tok, dw), bf16),
        V(lroot.shape, bf16),
        V(rroot.shape, bf16),
        pieces(own // rows, dw // width),
        pieces(COLS, nz),
        pieces(2, half),
        pieces(4, half),
        pieces(2, half),
        pieces(nz),
        pieces(max(nz - 1, 4)),
        pieces(mp),
        pieces(mp),
        pieces(2, COLS),
        pieces(COLS),
        pieces(COLS),
        pieces(2, nz),
        pieces(nz),
        pieces(nz),
        pieces(2, 2),
        pieces(2),
        V((128, width), f32),
        V((rows, width), f32),
        V((8, 128), f32),
        V((mp, 8, 128), f32),
        pieces(nz),
        pieces(nz),
        pieces(nz),
        pieces(3, COLS - 1),
        pieces(COLS),
        pieces(COLS),
        pieces(COLS),
        pieces(2 * cap + 1),
        D((10,)),
    ]
    for shape in [
        (2, COLS),
        (2, nz - 1),
        (2, 6),
        (2, max(nz - 1, 8)),
        (3, 2, 4),
        (3, ny),
        (mp - 1,),
        (3, 2, 4),
        (3, COLS - 1),
    ]:
        scratch += [D(shape), D(shape)]
    anywhere = pl.BlockSpec(memory_space=pltpu.HBM)
    result = pl.pallas_call(
        functools.partial(kernel, sizes),
        out_shape=jax.ShapeDtypeStruct((2 * cap + 1, rows, width), bf16),
        in_specs=[anywhere] * 6,
        out_specs=anywhere,
        scratch_shapes=scratch,
        compiler_params=pltpu.CompilerParams(collective_id=0, has_side_effects=True),
        name="shampoo",
    )(owner_map[None], owner_counts[None], acts, cot, lroot, rroot)
    return pl.pallas_call(
        finish,
        out_shape=(
            jax.ShapeDtypeStruct((1, rows, width), bf16),
            jax.ShapeDtypeStruct(lstat.shape, f32),
            jax.ShapeDtypeStruct(rstat.shape, f32),
        ),
        in_specs=[anywhere] * 3,
        out_specs=(anywhere,) * 3,
        scratch_shapes=[
            pieces(2 * cap + 1),
            V((2, *lstat.shape), f32),
            V((2, *lstat.shape), f32),
            D((3,)),
            D((3,)),
        ],
        name="finish",
    )(result, lstat, rstat)


def solution(mesh):
    in_specs = (
        P("dp", "mp"),
        P("dp", None),
        P("dp", "mp", None),
        P("dp", "mp", None),
        P("dp", "mp", None),
        P("dp", "mp", None),
        P(),
        P(),
    )
    out_specs = (P("dp", "mp", None), P("dp", "mp", None), P("dp", "mp", None))
    return jax.shard_map(shards, mesh=mesh, in_specs=in_specs, out_specs=out_specs, check_vma=False)
```

```python
import functools

import jax
import jax.numpy as jnp
from jax import lax
from jax.experimental import pallas as pl
from jax.experimental.pallas import tpu as pltpu
from jax.sharding import PartitionSpec as P

epsilon = 1e-06
COLS = 4
MESH = pl.DeviceIdType.MESH
PLANS = {
    1: (),
    2: ((0, 0, 1, False),),
    4: ((0, 0, 1, True), (0, 0, 2, False)),
    8: ((0, 0, 1, True), (0, 0, 2, True), (1, 2, 1, True), (1, 2, 2, False)),
}
f32, bf16 = jnp.float32, jnp.bfloat16


def kernel(
    sizes,
    omap,
    counts,
    acts,
    cot,
    lroot,
    rroot,
    result,
    om_v,
    ct_v,
    tab_v,
    tab,
    a_v,
    at_v,
    c_v,
    lr_v,
    rr_v,
    part,
    q,
    rel,
    xa,
    fwd,
    xsum,
    zr,
    gful,
    rful,
    rxs,
    rx_l,
    rx_r,
    rz_l,
    rz_r,
    rel_l,
    rel_r,
    fwd_l,
    fwd_r,
    got_l,
    got_r,
    zrel,
    zfwd,
    slab,
    ssq_s,
    ssq,
    ratio_s,
    ratio_z,
    ratio_xs,
    ratio_x,
    zb_l,
    zb_r,
    zb_u,
    fxs,
    fx_l,
    fx_r,
    fx_u,
    packed,
    loc,
    s_rx,
    r_rx,
    s_x,
    r_x,
    s_z,
    r_z,
    s_y,
    r_y,
    s_c,
    r_c,
    s_q,
    r_q,
    s_f,
    r_f,
    s_fx,
    r_fx,
    s_t,
    r_t,
):
    nz, ny, mp, rows, width, cap = sizes
    dp = lax.axis_index("dp")
    m = lax.axis_index("mp")
    x, z = dp % COLS, dp // COLS
    c, y = m % 2, m // 2
    half = nz // 2
    rx, rz, zb = (rx_l, rx_r), (rz_l, rz_r), (zb_l, zb_r, zb_u)
    fx = (fx_l, fx_r, fx_u)
    part_rows = [pl.ds(h * (rows // 2), rows // 2) for h in range(2)]

    def at_x(k):
        return {"dp": z * COLS + (x + k) % COLS}

    def at_z(k):
        return {"dp": ((z + k) % nz) * COLS + x}

    def at_y(k):
        return {"mp": ((y + k) % ny) * 2 + c}

    def at_m(k):
        return {"mp": (m + k) % mp}

    partner = {"mp": y * 2 + (1 - c)}

    def send(src, dst, ssem, rsem, where):
        return pltpu.make_async_remote_copy(
            src_ref=src,
            dst_ref=dst,
            send_sem=ssem,
            recv_sem=rsem,
            device_id=where,
            device_id_type=MESH,
        )

    def loop(lo, hi, body):
        def step(i, carry):
            body(i)
            return carry

        lax.fori_loop(lo, hi, step, 0)

    def spread(pos, n, where, ref, ssem, rsem):
        plan = PLANS[n]

        def copy(i, way):
            _, behind, hop, whole = plan[i]
            origin = (pos + n - behind) % n if way == 0 else (pos + behind) % n
            r = ref(origin, None if whole else way)
            return send(
                r, r, ssem.at[way, i], rsem.at[way, i], where(hop if way == 0 else n - hop)
            )

        def start(stage):
            for i, item in enumerate(plan):
                if item[0] == stage:
                    for way in range(2):
                        copy(i, way).start()

        def forward():
            if len(plan) > 2:
                for way in range(2):
                    copy(1, way).wait_recv()
                start(1)

        def finish(arrived=None):
            for i, item in enumerate(plan):
                for way in range(2):
                    if not (len(plan) > 2 and i == 1):
                        copy(i, way).wait_recv()
                if arrived is not None:
                    far = item[1] + item[2]
                    arrived(far)
                    if item[3]:
                        arrived(n - far)

        def drain():
            for i in range(len(plan)):
                for way in range(2):
                    copy(i, way).wait_send()

        return start, forward, finish, drain

    barrier = pltpu.get_barrier_semaphore()

    def hello(where):
        pl.semaphore_signal(barrier, inc=1, device_id=where, device_id_type=MESH)

    loads = [
        pltpu.make_async_copy(s, d, loc.at[i])
        for i, (s, d) in enumerate(
            [
                (lroot, lr_v),
                (rroot, rr_v),
                (acts, a_v),
                (cot, c_v),
                (omap, om_v),
                (counts, ct_v),
            ]
        )
    ]
    for i in (4, 5, 2, 3, 1, 0):
        loads[i].start()
    for k in range(1, COLS):
        hello(at_x(k))
    loop(1, nz, lambda k: hello(at_z(k)))
    loop(1, mp, lambda k: hello(at_m(k)))

    loads[4].wait()
    loads[5].wait()
    tables(om_v, ct_v, cap, tab_v)
    to_scalars = pltpu.make_async_copy(tab_v, tab, loc.at[6])
    to_scalars.start()

    loads[2].wait()
    tiles = a_v.shape[1] // 128
    each = 128 // rows

    def turn(i):
        columns = a_v[:, pl.ds(pl.multiple_of(i * 128, 128), 128)]
        at_v[pl.ds(i * each, each)] = columns.T.reshape(each, rows, a_v.shape[0])

    loop(0, tiles, turn)
    to_scalars.wait()
    def sum_z(src, near, fwd_z, got, n, at):
        def plain(k):
            return send(
                src.at[(z + k) % nz, at, :],
                got.at[k - 1, at, :],
                s_z.at[n, k - 1],
                r_z.at[n, k - 1],
                at_z(k),
            )

        def copy(way, kind):
            def there(k):
                return k if way == 0 else nz - k

            cols = pl.ds(way * (width // 2), width // 2)
            if kind == 0:
                a, b, k = src.at[(z + there(1)) % nz, at, :], got.at[way, at, :], 1
            elif kind == 1:
                a, b, k = src.at[(z + there(3)) % nz, at, :], near.at[way, 0, at, :], 1
            elif kind == 2:
                a, b, k = src.at[(z + there(4)) % nz, at, cols], near.at[way, 1, at, cols], 2
            else:
                a, b, k = fwd_z.at[way, at, :], got.at[2 + way, at, :], 2
            j = 4 * way + kind
            return send(a, b, s_z.at[n, j], r_z.at[n, j], at_z(there(k)))

        def start():
            if nz != 8:
                loop(1, nz, lambda k: plain(k).start())
                return
            for kind in (2, 1, 0):
                for way in range(2):
                    copy(way, kind).start()

        def onward():
            if nz != 8:
                return
            for way in range(2):
                cols = pl.ds(way * (width // 2), width // 2)
                copy(way, 1).wait_recv()
                copy(way, 2).wait_recv()
                to = (z + (2 if way == 0 else nz - 2)) % nz
                both = src[to, at, :].astype(f32) + near[way, 0, at, :].astype(f32)
                extra = near[way, 1, at, cols].astype(f32)
                none = jnp.zeros_like(extra)
                extra = jnp.concatenate([extra, none] if way == 0 else [none, extra], axis=1)
                fwd_z[way, at, :] = (both + extra).astype(bf16)
                copy(way, 3).start()

        def finish_z():
            total = src[z, at, :].astype(f32)
            if nz != 8:
                loop(1, nz, lambda k: plain(k).wait_recv())
                for k in range(nz - 1):
                    total = total + got[k, at, :].astype(f32)
                return total
            for way in range(2):
                copy(way, 0).wait_recv()
                copy(way, 3).wait_recv()
                total = total + got[way, at, :].astype(f32) + got[2 + way, at, :].astype(f32)
            return total

        def drain():
            if nz != 8:
                loop(1, nz, lambda k: plain(k).wait_send())
                return
            for way in range(2):
                for kind in range(4):
                    copy(way, kind).wait_send()

        return start, onward, finish_z, drain

    grad_z = [sum_z(xsum, zrel, zfwd, zr, h, part_rows[h]) for h in range(2)]
    every = pl.ds(0, rows)
    root_z = [
        sum_z(rz_l, rel_l, fwd_l, got_l, 2, every),
        sum_z(rz_r, rel_r, fwd_r, got_r, 3, every),
    ]

    loads[0].wait()
    loads[1].wait()
    start_me = tab[1, dp]

    def slot_for(col):
        return (col + 4 * COLS * nz - start_me) % COLS

    for k in range(COLS):
        r = slot_for((x + k) % COLS)
        rxs[0, k] = lr_v[r]
        rxs[1, k] = rr_v[r]
    rx_l[x] = rxs[0, 0]
    rx_r[x] = rxs[1, 0]

    def root_x(which, k):
        return send(
            rxs.at[which, k], rx[which].at[x], s_rx.at[which, k], r_rx.at[which, k], at_x(k)
        )

    def root_turn(which):
        for k in range(1, COLS):
            root_x(which, k).wait_recv()

        def root_row(row):
            owner = tab[3, row * COLS + x]
            block = rx[which][owner % COLS]
            rz[which][row] = jnp.where(owner // COLS == z, block, jnp.zeros_like(block))

        loop(0, nz, root_row)
        root_z[which][0]()

    pl.semaphore_wait(barrier, COLS - 1 + nz - 1 + mp - 1)
    for k in (2, 1, 3):
        root_x(1, k).start()
    loads[3].wait()

    wide = 256
    per = width // wide
    ncol = c_v.shape[1] // width

    def multiply(n):
        got = jnp.dot(
            at_v[...].reshape(-1, c_v.shape[0]),
            c_v[:, pl.ds(pl.multiple_of(n * wide, wide), wide)],
            preferred_element_type=f32,
        )
        got = got.astype(bf16).reshape(part.shape[0], rows, wide)
        part[:, n // per, :, pl.ds(pl.multiple_of((n % per) * wide, wide), wide)] = got

    def arrange(h):
        at = part_rows[h]

        def one(s):
            b = tab[2, s]
            q[s % COLS, s // COLS, at, :] = part[b // ncol, b % ncol, at, :]

        def row(k):
            for col in range(COLS):
                one(k * COLS + col)

        loop(0, nz, row)

    loop(0, c_v.shape[1] // wide, multiply)
    arrange(0)
    lo, hi = pl.ds(0, half), pl.ds(half, half)
    far, right, left = (x + 2) % COLS, (x + 1) % COLS, (x + 3) % COLS

    def x_copy(h, j, src, dst, k):
        return send(
            src.at[:, part_rows[h], :],
            dst.at[:, part_rows[h], :],
            s_x.at[h, j],
            r_x.at[h, j],
            at_x(k),
        )

    relay, direct, onward = [], [], []
    for h in range(2):
        relay.append(
            [
                x_copy(h, 0, q.at[far, lo], rel.at[0], 1),
                x_copy(h, 1, q.at[far, hi], rel.at[1], 3),
            ]
        )
        direct.append(
            [
                x_copy(h, 2, q.at[right, hi], xa.at[0], 1),
                x_copy(h, 3, q.at[left, lo], xa.at[1], 3),
            ]
        )
        onward.append(
            [x_copy(h, 4, fwd.at[0], xa.at[2], 1), x_copy(h, 5, fwd.at[1], xa.at[3], 3)]
        )
    for copy in relay[0] + direct[0]:
        copy.start()
    arrange(1)
    for copy in relay[1]:
        copy.start()

    def send_on(h):
        at = part_rows[h]
        for side, (toward, part_of) in enumerate([(right, lo), (left, hi)]):
            relay[h][side].wait_recv()
            fwd[side, :, at, :] = (
                q[toward, part_of, at, :].astype(f32) + rel[side, :, at, :].astype(f32)
            ).astype(bf16)
            onward[h][side].start()

    root_turn(1)
    send_on(0)
    for copy in direct[1]:
        copy.start()
    send_on(1)
    for k in range(1, COLS):
        root_x(0, k).start()

    def x_done(h):
        at = part_rows[h]
        for copy in direct[h] + onward[h]:
            copy.wait_recv()
        own = q[x, :, at, :].astype(f32)
        xsum[lo, at, :] = (
            own[:half] + xa[1, :, at, :].astype(f32) + xa[2, :, at, :].astype(f32)
        ).astype(bf16)
        xsum[hi, at, :] = (
            own[half:] + xa[0, :, at, :].astype(f32) + xa[3, :, at, :].astype(f32)
        ).astype(bf16)
        grad_z[h][0]()

    root_z[1][1]()
    x_done(0)
    x_done(1)

    grad_z[0][1]()
    rful[m] = root_z[1][2]().astype(bf16)

    def over_mp(full, j, at):
        def ref(origin, side):
            cols = slice(None) if side is None else pl.ds(side * (width // 2), width // 2)
            return full.at[origin * 2 + c, at, cols]

        def across(k):
            r = ref((y + ny - k) % ny, None)
            return send(r, r, s_c.at[j, k], r_c.at[j, k], partner)

        return spread(y, ny, at_y, ref, s_y.at[j], r_y.at[j]), across

    (r_start, r_forward, r_finish, r_drain), r_across = over_mp(rful, 2, pl.ds(0, rows))
    g_over = [over_mp(gful, h, part_rows[h]) for h in range(2)]
    r_start(0)
    r_across(0).start()
    grad_z[1][1]()
    root_turn(0)

    def z_done(h):
        gful[m, part_rows[h], :] = grad_z[h][2]().astype(bf16)
        (start, _, _, _), across = g_over[h]
        start(0)
        across(0).start()

    z_done(0)
    r_forward()
    z_done(1)
    g_over[0][0][1]()
    root_z[0][1]()
    g_over[1][0][1]()
    r_finish(lambda k: r_across(k).start())
    for h in range(2):
        (_, _, finish, _), across = g_over[h]
        finish(lambda k, across=across: across(k).start())
    for _, across in g_over:
        loop(0, ny, lambda k, across=across: across(k).wait_recv())
    loop(0, ny, lambda k: r_across(k).wait_recv())
    left_root = root_z[0][2]().astype(bf16)

    z_over = [
        spread(z, nz, at_z, lambda o, side, b=b: b.at[o] if side is None else b.at[o, :, pl.ds(side * (width // 2), width // 2)], s_f.at[i], r_f.at[i])
        for i, b in enumerate(zb)
    ]

    order = mp * rows
    g = gful[...].reshape(order, width)
    applied = jnp.dot(left_root, g, preferred_element_type=f32).astype(bf16)
    cond = jnp.dot(applied, rful[...].reshape(order, width), preferred_element_type=f32)
    zb_u[z] = cond.astype(bf16)
    z_over[2][0](0)
    partial_sum = jnp.broadcast_to(jnp.sum(cond * cond, keepdims=True), ssq_s.shape)
    ssq_s[...] = partial_sum
    ssq[m] = partial_sum

    def square_send(k):
        return send(ssq_s, ssq.at[m], s_q.at[k - 1], r_q.at[k - 1], at_m(k))

    loop(1, mp, lambda k: square_send(k).start())

    mine = gful[m]
    zb_l[z] = lax.dot_general(
        mine, g, (((1,), (1,)), ((), ())), preferred_element_type=f32
    ).astype(bf16)
    z_over[0][0](0)
    piece = pl.multiple_of((m * rows // 128) * 128, 128)
    columns = gful[:, :, pl.ds(piece, 128)].reshape(order, 128)
    slab[...] = lax.dot_general(columns, g, (((0,), (0,)), ((), ())), preferred_element_type=f32)
    zb_r[z] = slab[pl.ds((m * rows) % 128, rows), :].astype(bf16)
    z_over[1][0](0)
    wide_g = g.astype(f32)
    grad_square = jnp.sum(wide_g * wide_g, keepdims=True)
    z_over[2][1]()
    z_over[0][1]()
    loop(1, mp, lambda k: square_send(k).wait_recv())
    cond_square = jnp.sum(ssq[...], axis=0)[0:1, 0:1]
    entries = float(order * width)
    ratio = jnp.sqrt((grad_square / entries + epsilon) / (cond_square / entries + epsilon))
    ratio_s[...] = jnp.broadcast_to(ratio, ratio_s.shape)
    ratio_z[z] = jnp.broadcast_to(ratio, ratio_s.shape)

    def ratio_up(k):
        return send(ratio_s, ratio_z.at[z], s_t.at[0, k - 1], r_t.at[0, k - 1], at_z(k))

    def ratio_on(k):
        return send(
            ratio_xs.at[k - 1], ratio_x.at[x], s_t.at[1, k - 1], r_t.at[1, k - 1], at_x(k)
        )

    loop(1, nz, lambda k: ratio_up(k).start())
    z_over[1][1]()

    def seat_row(col):
        begin = tab[1, z * COLS + col]
        k = (begin + (x + 4 * COLS * nz - begin) % COLS) // COLS
        return jnp.minimum(k, nz - 1)

    def fin(j, k):
        return send(
            fxs.at[j, k - 1], fx[j].at[x], s_fx.at[j, k - 1], r_fx.at[j, k - 1], at_x(k)
        )

    def go_on(j):
        def pick(col):
            return zb[j][seat_row(col) if j < 2 else tab[0, z * COLS + col] // COLS]

        for k in (2, 1, 3):
            fxs[j, k - 1] = pick((x + k) % COLS)
            fin(j, k).start()
        fx[j][x] = pick(x)

    z_over[2][2]()
    go_on(2)
    z_over[0][2]()
    go_on(0)
    z_over[1][2]()
    go_on(1)
    for h in range(2):
        for copy in relay[h] + direct[h] + onward[h]:
            copy.wait_send()
        grad_z[h][3]()
        root_z[h][3]()
        g_over[h][0][3]()
        loop(0, ny, lambda k, h=h: g_over[h][1](k).wait_send())
        for k in range(1, COLS):
            root_x(h, k).wait_send()
    r_drain()
    loop(0, ny, lambda k: r_across(k).wait_send())
    loop(1, mp, lambda k: square_send(k).wait_send())
    for over in z_over:
        over[3]()
    loop(1, nz, lambda k: ratio_up(k).wait_recv())

    def ratio_for(col):
        return ratio_z[tab[0, z * COLS + col] // COLS]

    for k in (2, 1, 3):
        ratio_xs[k - 1] = ratio_for((x + k) % COLS)
        ratio_on(k).start()
    ratio_x[x] = ratio_for(x)
    loop(1, nz, lambda k: ratio_up(k).wait_send())
    limit = tab[4, dp]

    def put(j):
        at = pl.ds(j * cap, cap if j < 2 else 1)
        return pltpu.make_async_copy(packed.at[at], result.at[at], loc.at[7 + j])

    for j in range(2):
        for k in range(1, COLS):
            fin(j, k).wait_recv()
        for r in range(cap):
            add = fx[j][(start_me + r) % COLS]
            packed[j * cap + r] = jnp.where(limit > r, add, jnp.zeros_like(add))
        put(j).start()
    for k in range(1, COLS):
        fin(2, k).wait_recv()
        ratio_on(k).wait_recv()
    seat = tab[0, dp] % COLS
    home = fx[2][seat].astype(f32) * ratio_x[seat][0:1, 0:1]
    packed[2 * cap] = jnp.where(tab[5, dp] > 0, home, 0.0).astype(bf16)
    put(2).start()
    for k in range(1, COLS):
        ratio_on(k).wait_send()
        for j in range(3):
            fin(j, k).wait_send()
    for j in range(3):
        put(j).wait()


def finish(result, lstat, rstat, upd, new_left, new_right, packed, old, new, loc, out):
    cap = old.shape[1]
    get = [
        pltpu.make_async_copy(s, d, loc.at[i])
        for i, (s, d) in enumerate([(result, packed), (lstat, old.at[0]), (rstat, old.at[1])])
    ]
    for copy in get:
        copy.start()
    get[0].wait()
    put = [pltpu.make_async_copy(packed.at[pl.ds(2 * cap, 1)], upd, out.at[0])]
    put[0].start()
    for j, to in enumerate([new_left, new_right]):
        get[1 + j].wait()
        new[j] = old[j] + packed[pl.ds(j * cap, cap)].astype(f32)
        copy = pltpu.make_async_copy(new.at[j], to, out.at[1 + j])
        copy.start()
        put.append(copy)
    for copy in put:
        copy.wait()


def tables(omap, counts, capacity, out):
    blocks = omap.shape[1]
    shape = (blocks, blocks)
    i = lax.broadcasted_iota(jnp.int32, shape, 0)
    j = lax.broadcasted_iota(jnp.int32, shape, 1)

    def over_i(value):
        return jnp.sum(value.astype(jnp.int32), axis=0, keepdims=True)

    def over_j(value):
        return jnp.sum(value.astype(jnp.int32), axis=1, keepdims=True)

    row = jnp.broadcast_to(omap[...], shape)
    many = jnp.broadcast_to(counts[...], shape)
    col = jnp.broadcast_to(over_j(jnp.where(i == j, row, 0)), shape)
    many_col = jnp.broadcast_to(over_j(jnp.where(i == j, many, 0)), shape)
    rank = over_i(jnp.where((col == row) & (i < j), 1, 0))
    place = over_i(jnp.where(col < row, 1, 0)) + rank
    place_col = over_j(jnp.where((row < col) | ((row == col) & (j < i)), 1, 0))
    at = jnp.broadcast_to(place_col, shape) == j
    limit = jnp.minimum(over_i(jnp.where(col == j, 1, 0)), counts[...])
    held = over_i(jnp.where(row == i, many_col, 0))
    live = jnp.where((rank < held) & (rank < capacity), 1, 0)
    for n, value in enumerate(
        [
            place,
            over_i(jnp.where(col < j, 1, 0)),
            over_i(jnp.where(at, i, 0)),
            over_i(jnp.where(at, col, 0)),
            jnp.minimum(limit, capacity),
            live,
        ]
    ):
        out[n : n + 1, 0:blocks] = value


def shards(acts, cot, lstat, rstat, lroot, rroot, owner_map, owner_counts):
    cap, rows, width = lstat.shape
    tok, own = acts.shape
    dw = cot.shape[1]
    devices, mp = lax.axis_size("dp"), lax.axis_size("mp")
    nz, ny = devices // COLS, mp // 2
    sizes = (nz, ny, mp, rows, width, cap)
    V, D = pltpu.VMEM, pltpu.SemaphoreType.DMA
    half = nz // 2

    def pieces(*lead):
        return V((*lead, rows, width), bf16)

    scratch = [
        V((1, devices), jnp.int32),
        V((1, devices), jnp.int32),
        V((8, 128), jnp.int32),
        pltpu.SMEM((8, 128), jnp.int32),
        V((tok, own), bf16),
        V((own // rows, rows, tok), bf16),
        V((tok, dw), bf16),
        V(lroot.shape, bf16),
        V(rroot.shape, bf16),
        pieces(own // rows, dw // width),
        pieces(COLS, nz),
        pieces(2, half),
        pieces(4, half),
        pieces(2, half),
        pieces(nz),
        pieces(max(nz - 1, 4)),
        pieces(mp),
        pieces(mp),
        pieces(2, COLS),
        pieces(COLS),
        pieces(COLS),
        pieces(nz),
        pieces(nz),
        pieces(2, 2),
        pieces(2, 2),
        pieces(2),
        pieces(2),
        pieces(max(nz - 1, 4)),
        pieces(max(nz - 1, 4)),
        pieces(2, 2),
        pieces(2),
        V((128, width), f32),
        V((8, 128), f32),
        V((mp, 8, 128), f32),
        V((8, 128), f32),
        V((nz, 8, 128), f32),
        V((COLS - 1, 8, 128), f32),
        V((COLS, 8, 128), f32),
        pieces(nz),
        pieces(nz),
        pieces(nz),
        pieces(3, COLS - 1),
        pieces(COLS),
        pieces(COLS),
        pieces(COLS),
        pieces(2 * cap + 1),
        D((10,)),
    ]
    for shape in [
        (2, COLS),
        (2, 6),
        (4, max(nz - 1, 8)),
        (3, 2, 4),
        (3, ny),
        (mp - 1,),
        (3, 2, 4),
        (3, COLS - 1),
        (2, max(nz - 1, COLS - 1)),
    ]:
        scratch += [D(shape), D(shape)]
    anywhere = pl.BlockSpec(memory_space=pltpu.HBM)
    result = pl.pallas_call(
        functools.partial(kernel, sizes),
        out_shape=jax.ShapeDtypeStruct((2 * cap + 1, rows, width), bf16),
        in_specs=[anywhere] * 6,
        out_specs=anywhere,
        scratch_shapes=scratch,
        compiler_params=pltpu.CompilerParams(collective_id=0, has_side_effects=True),
        name="shampoo",
    )(owner_map[None], owner_counts[None], acts, cot, lroot, rroot)
    return pl.pallas_call(
        finish,
        out_shape=(
            jax.ShapeDtypeStruct((1, rows, width), bf16),
            jax.ShapeDtypeStruct(lstat.shape, f32),
            jax.ShapeDtypeStruct(rstat.shape, f32),
        ),
        in_specs=[anywhere] * 3,
        out_specs=(anywhere,) * 3,
        scratch_shapes=[
            pieces(2 * cap + 1),
            V((2, *lstat.shape), f32),
            V((2, *lstat.shape), f32),
            D((3,)),
            D((3,)),
        ],
        name="finish",
    )(result, lstat, rstat)


def solution(mesh):
    in_specs = (
        P("dp", "mp"),
        P("dp", None),
        P("dp", "mp", None),
        P("dp", "mp", None),
        P("dp", "mp", None),
        P("dp", "mp", None),
        P(),
        P(),
    )
    out_specs = (P("dp", "mp", None), P("dp", "mp", None), P("dp", "mp", None))
    return jax.shard_map(shards, mesh=mesh, in_specs=in_specs, out_specs=out_specs, check_vma=False)
```

```python
import functools

import jax
import jax.numpy as jnp
from jax import lax
from jax.experimental import pallas as pl
from jax.experimental.pallas import tpu as pltpu
from jax.sharding import PartitionSpec as P

epsilon = 1e-06
COLS = 4
MESH = pl.DeviceIdType.MESH
PLANS = {
    1: (),
    2: ((0, 0, 1, False),),
    4: ((0, 0, 1, True), (0, 0, 2, False)),
    8: ((0, 0, 1, True), (0, 0, 2, True), (1, 2, 1, True), (1, 2, 2, False)),
}
f32, bf16 = jnp.float32, jnp.bfloat16


def kernel(
    sizes,
    omap,
    counts,
    acts,
    cot,
    lroot,
    rroot,
    result,
    om_v,
    ct_v,
    tab_v,
    tab,
    a_v,
    at_v,
    c_v,
    lr_v,
    rr_v,
    part,
    q,
    rel,
    xa,
    fwd,
    xsum,
    zr,
    gful,
    rful,
    rxs,
    rx_l,
    rx_r,
    rz_l,
    rz_r,
    rel_l,
    rel_r,
    fwd_l,
    fwd_r,
    got_l,
    got_r,
    zrel,
    zfwd,
    slab,
    ssq_s,
    ssq,
    ratio_s,
    ratio_z,
    ratio_xs,
    ratio_x,
    zb_l,
    zb_r0,
    zb_r1,
    zb_u,
    fxs_l,
    fxs_r0,
    fxs_r1,
    fxs_u,
    fx_l,
    fx_r0,
    fx_r1,
    fx_u,
    packed,
    loc,
    s_rx,
    r_rx,
    s_x,
    r_x,
    s_z,
    r_z,
    s_y,
    r_y,
    s_c,
    r_c,
    s_q,
    r_q,
    s_f,
    r_f,
    s_fx,
    r_fx,
    s_t,
    r_t,
):
    nz, ny, mp, rows, width, cap = sizes
    dp = lax.axis_index("dp")
    m = lax.axis_index("mp")
    x, z = dp % COLS, dp // COLS
    c, y = m % 2, m // 2
    half = nz // 2
    rx, rz, zb = (rx_l, rx_r), (rz_l, rz_r), (zb_l, zb_r0, zb_r1, zb_u)
    fx = (fx_l, fx_r0, fx_r1, fx_u)
    fxs = (fxs_l, fxs_r0, fxs_r1, fxs_u)
    part_rows = [pl.ds(h * (rows // 2), rows // 2) for h in range(2)]

    def at_x(k):
        return {"dp": z * COLS + (x + k) % COLS}

    def at_z(k):
        return {"dp": ((z + k) % nz) * COLS + x}

    def at_y(k):
        return {"mp": ((y + k) % ny) * 2 + c}

    def at_m(k):
        return {"mp": (m + k) % mp}

    partner = {"mp": y * 2 + (1 - c)}

    def send(src, dst, ssem, rsem, where):
        return pltpu.make_async_remote_copy(
            src_ref=src,
            dst_ref=dst,
            send_sem=ssem,
            recv_sem=rsem,
            device_id=where,
            device_id_type=MESH,
        )

    def loop(lo, hi, body):
        def step(i, carry):
            body(i)
            return carry

        lax.fori_loop(lo, hi, step, 0)

    def spread(pos, n, where, ref, ssem, rsem):
        plan = PLANS[n]

        def copy(i, way):
            _, behind, hop, whole = plan[i]
            origin = (pos + n - behind) % n if way == 0 else (pos + behind) % n
            r = ref(origin, None if whole else way)
            return send(
                r, r, ssem.at[way, i], rsem.at[way, i], where(hop if way == 0 else n - hop)
            )

        def start(stage):
            for i, item in enumerate(plan):
                if item[0] == stage:
                    for way in range(2):
                        copy(i, way).start()

        def forward():
            if len(plan) > 2:
                for way in range(2):
                    copy(1, way).wait_recv()
                start(1)

        def finish(arrived=None):
            for i, item in enumerate(plan):
                for way in range(2):
                    if not (len(plan) > 2 and i == 1):
                        copy(i, way).wait_recv()
                if arrived is not None:
                    far = item[1] + item[2]
                    arrived(far)
                    if item[3]:
                        arrived(n - far)

        def drain():
            for i in range(len(plan)):
                for way in range(2):
                    copy(i, way).wait_send()

        return start, forward, finish, drain

    barrier = pltpu.get_barrier_semaphore()

    def hello(where):
        pl.semaphore_signal(barrier, inc=1, device_id=where, device_id_type=MESH)

    loads = [
        pltpu.make_async_copy(s, d, loc.at[i])
        for i, (s, d) in enumerate(
            [
                (lroot, lr_v),
                (rroot, rr_v),
                (acts, a_v),
                (cot, c_v),
                (omap, om_v),
                (counts, ct_v),
            ]
        )
    ]
    for i in (4, 5, 2, 3, 1, 0):
        loads[i].start()
    for k in range(1, COLS):
        hello(at_x(k))
    loop(1, nz, lambda k: hello(at_z(k)))
    loop(1, mp, lambda k: hello(at_m(k)))

    loads[4].wait()
    loads[5].wait()
    tables(om_v, ct_v, cap, tab_v)
    to_scalars = pltpu.make_async_copy(tab_v, tab, loc.at[6])
    to_scalars.start()

    loads[2].wait()
    tiles = a_v.shape[1] // 128
    each = 128 // rows

    def turn(i):
        columns = a_v[:, pl.ds(pl.multiple_of(i * 128, 128), 128)]
        at_v[pl.ds(i * each, each)] = columns.T.reshape(each, rows, a_v.shape[0])

    loop(0, tiles, turn)
    to_scalars.wait()
    def sum_z(src, near, fwd_z, got, n, at):
        def plain(k):
            return send(
                src.at[(z + k) % nz, at, :],
                got.at[k - 1, at, :],
                s_z.at[n, k - 1],
                r_z.at[n, k - 1],
                at_z(k),
            )

        def copy(way, kind):
            def there(k):
                return k if way == 0 else nz - k

            cols = pl.ds(way * (width // 2), width // 2)
            if kind == 0:
                a, b, k = src.at[(z + there(1)) % nz, at, :], got.at[way, at, :], 1
            elif kind == 1:
                a, b, k = src.at[(z + there(3)) % nz, at, :], near.at[way, 0, at, :], 1
            elif kind == 2:
                a, b, k = src.at[(z + there(4)) % nz, at, cols], near.at[way, 1, at, cols], 2
            else:
                a, b, k = fwd_z.at[way, at, :], got.at[2 + way, at, :], 2
            j = 4 * way + kind
            return send(a, b, s_z.at[n, j], r_z.at[n, j], at_z(there(k)))

        def start():
            if nz != 8:
                loop(1, nz, lambda k: plain(k).start())
                return
            for kind in (2, 1, 0):
                for way in range(2):
                    copy(way, kind).start()

        def onward():
            if nz != 8:
                return
            for way in range(2):
                cols = pl.ds(way * (width // 2), width // 2)
                copy(way, 1).wait_recv()
                copy(way, 2).wait_recv()
                to = (z + (2 if way == 0 else nz - 2)) % nz
                both = src[to, at, :].astype(f32) + near[way, 0, at, :].astype(f32)
                extra = near[way, 1, at, cols].astype(f32)
                none = jnp.zeros_like(extra)
                extra = jnp.concatenate([extra, none] if way == 0 else [none, extra], axis=1)
                fwd_z[way, at, :] = (both + extra).astype(bf16)
                copy(way, 3).start()

        def finish_z():
            total = src[z, at, :].astype(f32)
            if nz != 8:
                loop(1, nz, lambda k: plain(k).wait_recv())
                for k in range(nz - 1):
                    total = total + got[k, at, :].astype(f32)
                return total
            for way in range(2):
                copy(way, 0).wait_recv()
                copy(way, 3).wait_recv()
                total = total + got[way, at, :].astype(f32) + got[2 + way, at, :].astype(f32)
            return total

        def drain():
            if nz != 8:
                loop(1, nz, lambda k: plain(k).wait_send())
                return
            for way in range(2):
                for kind in range(4):
                    copy(way, kind).wait_send()

        return start, onward, finish_z, drain

    grad_z = [sum_z(xsum, zrel, zfwd, zr, h, part_rows[h]) for h in range(2)]
    every = pl.ds(0, rows)
    root_z = [
        sum_z(rz_l, rel_l, fwd_l, got_l, 2, every),
        sum_z(rz_r, rel_r, fwd_r, got_r, 3, every),
    ]

    loads[0].wait()
    loads[1].wait()
    start_me = tab[1, dp]

    def slot_for(col):
        return (col + 4 * COLS * nz - start_me) % COLS

    for k in range(COLS):
        r = slot_for((x + k) % COLS)
        rxs[0, k] = lr_v[r]
        rxs[1, k] = rr_v[r]
    rx_l[x] = rxs[0, 0]
    rx_r[x] = rxs[1, 0]

    def root_x(which, k):
        return send(
            rxs.at[which, k], rx[which].at[x], s_rx.at[which, k], r_rx.at[which, k], at_x(k)
        )

    def root_turn(which):
        for k in range(1, COLS):
            root_x(which, k).wait_recv()

        def root_row(row):
            owner = tab[3, row * COLS + x]
            block = rx[which][owner % COLS]
            rz[which][row] = jnp.where(owner // COLS == z, block, jnp.zeros_like(block))

        loop(0, nz, root_row)
        root_z[which][0]()

    pl.semaphore_wait(barrier, COLS - 1 + nz - 1 + mp - 1)
    for k in (2, 1, 3):
        root_x(1, k).start()
    loads[3].wait()

    wide = 256
    per = width // wide
    ncol = c_v.shape[1] // width

    def multiply(n):
        got = jnp.dot(
            at_v[...].reshape(-1, c_v.shape[0]),
            c_v[:, pl.ds(pl.multiple_of(n * wide, wide), wide)],
            preferred_element_type=f32,
        )
        got = got.astype(bf16).reshape(part.shape[0], rows, wide)
        part[:, n // per, :, pl.ds(pl.multiple_of((n % per) * wide, wide), wide)] = got

    def arrange(h, *cols):
        at = part_rows[h]

        def row(k):
            for col in cols:
                b = tab[2, k * COLS + col]
                q[col, k, at, :] = part[b // ncol, b % ncol, at, :]

        loop(0, nz, row)

    loop(0, c_v.shape[1] // wide, multiply)
    lo, hi = pl.ds(0, half), pl.ds(half, half)
    far, right, left = (x + 2) % COLS, (x + 1) % COLS, (x + 3) % COLS

    def x_copy(h, j, src, dst, k):
        return send(
            src.at[:, part_rows[h], :],
            dst.at[:, part_rows[h], :],
            s_x.at[h, j],
            r_x.at[h, j],
            at_x(k),
        )

    relay, direct, onward = [], [], []
    for h in range(2):
        relay.append(
            [
                x_copy(h, 0, q.at[far, lo], rel.at[0], 1),
                x_copy(h, 1, q.at[far, hi], rel.at[1], 3),
            ]
        )
        direct.append(
            [
                x_copy(h, 2, q.at[right, hi], xa.at[0], 1),
                x_copy(h, 3, q.at[left, lo], xa.at[1], 3),
            ]
        )
        onward.append(
            [x_copy(h, 4, fwd.at[0], xa.at[2], 1), x_copy(h, 5, fwd.at[1], xa.at[3], 3)]
        )
    for h in range(2):
        arrange(h, far)
        for copy in relay[h]:
            copy.start()
        arrange(h, right, left)
        if h == 0:
            for copy in direct[0]:
                copy.start()
    arrange(0, x)
    arrange(1, x)

    def send_on(h):
        at = part_rows[h]
        for side, (toward, part_of) in enumerate([(right, lo), (left, hi)]):
            relay[h][side].wait_recv()
            fwd[side, :, at, :] = (
                q[toward, part_of, at, :].astype(f32) + rel[side, :, at, :].astype(f32)
            ).astype(bf16)
            onward[h][side].start()

    root_turn(1)
    send_on(0)
    for copy in direct[1]:
        copy.start()
    send_on(1)
    for k in range(1, COLS):
        root_x(0, k).start()

    def x_done(h):
        at = part_rows[h]
        for copy in direct[h] + onward[h]:
            copy.wait_recv()
        own = q[x, :, at, :].astype(f32)
        xsum[lo, at, :] = (
            own[:half] + xa[1, :, at, :].astype(f32) + xa[2, :, at, :].astype(f32)
        ).astype(bf16)
        xsum[hi, at, :] = (
            own[half:] + xa[0, :, at, :].astype(f32) + xa[3, :, at, :].astype(f32)
        ).astype(bf16)
        grad_z[h][0]()

    root_z[1][1]()
    x_done(0)
    x_done(1)

    grad_z[0][1]()
    rful[m] = root_z[1][2]().astype(bf16)

    def over_mp(full, j, at):
        def ref(origin, side):
            cols = slice(None) if side is None else pl.ds(side * (width // 2), width // 2)
            return full.at[origin * 2 + c, at, cols]

        def across(k):
            r = ref((y + ny - k) % ny, None)
            return send(r, r, s_c.at[j, k], r_c.at[j, k], partner)

        return spread(y, ny, at_y, ref, s_y.at[j], r_y.at[j]), across

    (r_start, r_forward, r_finish, r_drain), r_across = over_mp(rful, 2, pl.ds(0, rows))
    g_over = [over_mp(gful, h, part_rows[h]) for h in range(2)]
    r_start(0)
    r_across(0).start()
    grad_z[1][1]()
    root_turn(0)

    def z_done(h):
        gful[m, part_rows[h], :] = grad_z[h][2]().astype(bf16)
        (start, _, _, _), across = g_over[h]
        start(0)
        across(0).start()

    z_done(0)
    r_forward()
    z_done(1)
    g_over[0][0][1]()
    root_z[0][1]()
    g_over[1][0][1]()
    r_finish(lambda k: r_across(k).start())
    for h in range(2):
        (_, _, finish, _), across = g_over[h]
        finish(lambda k, across=across: across(k).start())
    for _, across in g_over:
        loop(0, ny, lambda k, across=across: across(k).wait_recv())
    loop(0, ny, lambda k: r_across(k).wait_recv())
    left_root = root_z[0][2]().astype(bf16)

    z_over = [
        spread(z, nz, at_z, lambda o, side, b=b: b.at[o] if side is None else b.at[o, :, pl.ds(side * (width // 2), width // 2)], s_f.at[i], r_f.at[i])
        for i, b in enumerate(zb)
    ]

    order = mp * rows
    g = gful[...].reshape(order, width)
    applied = jnp.dot(left_root, g, preferred_element_type=f32).astype(bf16)
    cond = jnp.dot(applied, rful[...].reshape(order, width), preferred_element_type=f32)
    zb_u[z] = cond.astype(bf16)
    z_over[3][0](0)
    partial_sum = jnp.broadcast_to(jnp.sum(cond * cond, keepdims=True), ssq_s.shape)
    ssq_s[...] = partial_sum
    ssq[m] = partial_sum

    def square_send(k):
        return send(ssq_s, ssq.at[m], s_q.at[k - 1], r_q.at[k - 1], at_m(k))

    loop(1, mp, lambda k: square_send(k).start())

    mine = gful[m]
    zb_l[z] = lax.dot_general(
        mine, g, (((1,), (1,)), ((), ())), preferred_element_type=f32
    ).astype(bf16)
    z_over[0][0](0)
    piece = pl.multiple_of((m * rows // 128) * 128, 128)
    columns = gful[:, :, pl.ds(piece, 128)].reshape(order, 128)
    slab[...] = lax.dot_general(columns, g, (((0,), (0,)), ((), ())), preferred_element_type=f32)
    for h, place in enumerate((zb_r0, zb_r1)):
        at = pl.ds((m * rows) % 128 + h * (rows // 2), rows // 2)
        place[z] = slab[at, :].astype(bf16)
        z_over[1 + h][0](0)
    wide_g = g.astype(f32)
    grad_square = jnp.sum(wide_g * wide_g, keepdims=True)
    z_over[3][1]()
    z_over[0][1]()
    loop(1, mp, lambda k: square_send(k).wait_recv())
    cond_square = jnp.sum(ssq[...], axis=0)[0:1, 0:1]
    entries = float(order * width)
    ratio = jnp.sqrt((grad_square / entries + epsilon) / (cond_square / entries + epsilon))
    ratio_s[...] = jnp.broadcast_to(ratio, ratio_s.shape)
    ratio_z[z] = jnp.broadcast_to(ratio, ratio_s.shape)

    def ratio_up(k):
        return send(ratio_s, ratio_z.at[z], s_t.at[0, k - 1], r_t.at[0, k - 1], at_z(k))

    def ratio_on(k):
        return send(
            ratio_xs.at[k - 1], ratio_x.at[x], s_t.at[1, k - 1], r_t.at[1, k - 1], at_x(k)
        )

    loop(1, nz, lambda k: ratio_up(k).start())
    z_over[1][1]()
    z_over[2][1]()

    def seat_row(col):
        begin = tab[1, z * COLS + col]
        k = (begin + (x + 4 * COLS * nz - begin) % COLS) // COLS
        return jnp.minimum(k, nz - 1)

    def fin(j, k):
        return send(
            fxs[j].at[k - 1], fx[j].at[x], s_fx.at[j, k - 1], r_fx.at[j, k - 1], at_x(k)
        )

    def go_on(j):
        def pick(col):
            return zb[j][seat_row(col) if j < 3 else tab[0, z * COLS + col] // COLS]

        for k in (2, 1, 3):
            fxs[j][k - 1] = pick((x + k) % COLS)
            fin(j, k).start()
        fx[j][x] = pick(x)

    z_over[3][2]()
    go_on(3)
    z_over[0][2]()
    go_on(0)
    z_over[1][2]()
    go_on(1)
    z_over[2][2]()
    go_on(2)
    for h in range(2):
        for copy in relay[h] + direct[h] + onward[h]:
            copy.wait_send()
        grad_z[h][3]()
        root_z[h][3]()
        g_over[h][0][3]()
        loop(0, ny, lambda k, h=h: g_over[h][1](k).wait_send())
        for k in range(1, COLS):
            root_x(h, k).wait_send()
    r_drain()
    loop(0, ny, lambda k: r_across(k).wait_send())
    loop(1, mp, lambda k: square_send(k).wait_send())
    for over in z_over:
        over[3]()
    loop(1, nz, lambda k: ratio_up(k).wait_recv())

    def ratio_for(col):
        return ratio_z[tab[0, z * COLS + col] // COLS]

    for k in (2, 1, 3):
        ratio_xs[k - 1] = ratio_for((x + k) % COLS)
        ratio_on(k).start()
    ratio_x[x] = ratio_for(x)
    loop(1, nz, lambda k: ratio_up(k).wait_send())
    limit = tab[4, dp]

    def put(j):
        at = pl.ds(j * cap, cap if j < 2 else 1)
        return pltpu.make_async_copy(packed.at[at], result.at[at], loc.at[7 + j])

    for j in range(3):
        for k in range(1, COLS):
            fin(j, k).wait_recv()
        at = every if j == 0 else part_rows[j - 1]
        for r in range(cap):
            add = fx[j][(start_me + r) % COLS]
            packed[min(j, 1) * cap + r, at, :] = jnp.where(limit > r, add, jnp.zeros_like(add))
        if j != 1:
            put(min(j, 1)).start()
    for k in range(1, COLS):
        fin(3, k).wait_recv()
        ratio_on(k).wait_recv()
    seat = tab[0, dp] % COLS
    home = fx[3][seat].astype(f32) * ratio_x[seat][0:1, 0:1]
    packed[2 * cap] = jnp.where(tab[5, dp] > 0, home, 0.0).astype(bf16)
    put(2).start()
    for k in range(1, COLS):
        ratio_on(k).wait_send()
        for j in range(4):
            fin(j, k).wait_send()
    for j in range(3):
        put(j).wait()


def finish(result, lstat, rstat, upd, new_left, new_right, packed, old, new, loc, out):
    cap = old.shape[1]
    get = [
        pltpu.make_async_copy(s, d, loc.at[i])
        for i, (s, d) in enumerate([(result, packed), (lstat, old.at[0]), (rstat, old.at[1])])
    ]
    for copy in get:
        copy.start()
    get[0].wait()
    put = [pltpu.make_async_copy(packed.at[pl.ds(2 * cap, 1)], upd, out.at[0])]
    put[0].start()
    for j, to in enumerate([new_left, new_right]):
        get[1 + j].wait()
        new[j] = old[j] + packed[pl.ds(j * cap, cap)].astype(f32)
        copy = pltpu.make_async_copy(new.at[j], to, out.at[1 + j])
        copy.start()
        put.append(copy)
    for copy in put:
        copy.wait()


def tables(omap, counts, capacity, out):
    blocks = omap.shape[1]
    shape = (blocks, blocks)
    i = lax.broadcasted_iota(jnp.int32, shape, 0)
    j = lax.broadcasted_iota(jnp.int32, shape, 1)

    def over_i(value):
        return jnp.sum(value.astype(jnp.int32), axis=0, keepdims=True)

    def over_j(value):
        return jnp.sum(value.astype(jnp.int32), axis=1, keepdims=True)

    row = jnp.broadcast_to(omap[...], shape)
    many = jnp.broadcast_to(counts[...], shape)
    col = jnp.broadcast_to(over_j(jnp.where(i == j, row, 0)), shape)
    many_col = jnp.broadcast_to(over_j(jnp.where(i == j, many, 0)), shape)
    rank = over_i(jnp.where((col == row) & (i < j), 1, 0))
    place = over_i(jnp.where(col < row, 1, 0)) + rank
    place_col = over_j(jnp.where((row < col) | ((row == col) & (j < i)), 1, 0))
    at = jnp.broadcast_to(place_col, shape) == j
    limit = jnp.minimum(over_i(jnp.where(col == j, 1, 0)), counts[...])
    held = over_i(jnp.where(row == i, many_col, 0))
    live = jnp.where((rank < held) & (rank < capacity), 1, 0)
    for n, value in enumerate(
        [
            place,
            over_i(jnp.where(col < j, 1, 0)),
            over_i(jnp.where(at, i, 0)),
            over_i(jnp.where(at, col, 0)),
            jnp.minimum(limit, capacity),
            live,
        ]
    ):
        out[n : n + 1, 0:blocks] = value


def shards(acts, cot, lstat, rstat, lroot, rroot, owner_map, owner_counts):
    cap, rows, width = lstat.shape
    tok, own = acts.shape
    dw = cot.shape[1]
    devices, mp = lax.axis_size("dp"), lax.axis_size("mp")
    nz, ny = devices // COLS, mp // 2
    sizes = (nz, ny, mp, rows, width, cap)
    V, D = pltpu.VMEM, pltpu.SemaphoreType.DMA
    half = nz // 2

    def pieces(*lead):
        return V((*lead, rows, width), bf16)

    scratch = [
        V((1, devices), jnp.int32),
        V((1, devices), jnp.int32),
        V((8, 128), jnp.int32),
        pltpu.SMEM((8, 128), jnp.int32),
        V((tok, own), bf16),
        V((own // rows, rows, tok), bf16),
        V((tok, dw), bf16),
        V(lroot.shape, bf16),
        V(rroot.shape, bf16),
        pieces(own // rows, dw // width),
        pieces(COLS, nz),
        pieces(2, half),
        pieces(4, half),
        pieces(2, half),
        pieces(nz),
        pieces(max(nz - 1, 4)),
        pieces(mp),
        pieces(mp),
        pieces(2, COLS),
        pieces(COLS),
        pieces(COLS),
        pieces(nz),
        pieces(nz),
        pieces(2, 2),
        pieces(2, 2),
        pieces(2),
        pieces(2),
        pieces(max(nz - 1, 4)),
        pieces(max(nz - 1, 4)),
        pieces(2, 2),
        pieces(2),
        V((128, width), f32),
        V((8, 128), f32),
        V((mp, 8, 128), f32),
        V((8, 128), f32),
        V((nz, 8, 128), f32),
        V((COLS - 1, 8, 128), f32),
        V((COLS, 8, 128), f32),
        pieces(nz),
        V((nz, rows // 2, width), bf16),
        V((nz, rows // 2, width), bf16),
        pieces(nz),
        pieces(COLS - 1),
        V((COLS - 1, rows // 2, width), bf16),
        V((COLS - 1, rows // 2, width), bf16),
        pieces(COLS - 1),
        pieces(COLS),
        V((COLS, rows // 2, width), bf16),
        V((COLS, rows // 2, width), bf16),
        pieces(COLS),
        pieces(2 * cap + 1),
        D((10,)),
    ]
    for shape in [
        (2, COLS),
        (2, 6),
        (4, max(nz - 1, 8)),
        (3, 2, 4),
        (3, ny),
        (mp - 1,),
        (4, 2, 4),
        (4, COLS - 1),
        (2, max(nz - 1, COLS - 1)),
    ]:
        scratch += [D(shape), D(shape)]
    anywhere = pl.BlockSpec(memory_space=pltpu.HBM)
    result = pl.pallas_call(
        functools.partial(kernel, sizes),
        out_shape=jax.ShapeDtypeStruct((2 * cap + 1, rows, width), bf16),
        in_specs=[anywhere] * 6,
        out_specs=anywhere,
        scratch_shapes=scratch,
        compiler_params=pltpu.CompilerParams(collective_id=0, has_side_effects=True),
        name="shampoo",
    )(owner_map[None], owner_counts[None], acts, cot, lroot, rroot)
    return pl.pallas_call(
        finish,
        out_shape=(
            jax.ShapeDtypeStruct((1, rows, width), bf16),
            jax.ShapeDtypeStruct(lstat.shape, f32),
            jax.ShapeDtypeStruct(rstat.shape, f32),
        ),
        in_specs=[anywhere] * 3,
        out_specs=(anywhere,) * 3,
        scratch_shapes=[
            pieces(2 * cap + 1),
            V((2, *lstat.shape), f32),
            V((2, *lstat.shape), f32),
            D((3,)),
            D((3,)),
        ],
        name="finish",
    )(result, lstat, rstat)


def solution(mesh):
    in_specs = (
        P("dp", "mp"),
        P("dp", None),
        P("dp", "mp", None),
        P("dp", "mp", None),
        P("dp", "mp", None),
        P("dp", "mp", None),
        P(),
        P(),
    )
    out_specs = (P("dp", "mp", None), P("dp", "mp", None), P("dp", "mp", None))
    return jax.shard_map(shards, mesh=mesh, in_specs=in_specs, out_specs=out_specs, check_vma=False)
```
